8 devices in a mesh: tp: 4 (over z, y, x), cp: 2 (over core).
Axes of the slice: x: 2, y: 2, z: 1, core: 2. Of those that a mesh axis runs over, the one named last changes fastest.
Arguments:
- tokens: int32 [2048], P('cp')
- pos: int32 [2048], P('cp')
- doc_id: int32 [2048], P('cp')
- dy: bfloat16 [2048, 2048], P('cp')
- table: bfloat16 [32000, 2048], P('tp')
- w_q: bfloat16 [2048, 2048], P(None, 'tp')
- w_k: bfloat16 [2048, 2048], P(None, 'tp')
- w_v: bfloat16 [2048, 2048], P(None, 'tp')
- w_o: bfloat16 [2048, 2048], P('tp')
- w_gate: bfloat16 [2048, 5504], P(None, 'tp')
- w_up: bfloat16 [2048, 5504], P(None, 'tp')
- w_down: bfloat16 [5504, 2048], P('tp')
- gain_one: bfloat16 [2048], replicated
- gain_two: bfloat16 [2048], replicated
- inv_freq: float32 [64], replicated
Outputs:
- output 1: bfloat16 [2048, 2048], P('cp')
- output 2: float32 [32000, 2048], P('tp')
- output 3: float32 [2048, 2048], P(None, 'tp')
- output 4: float32 [2048, 2048], P(None, 'tp')
- output 5: float32 [2048, 2048], P(None, 'tp')
- output 6: float32 [2048, 2048], P('tp')
- output 7: float32 [2048, 5504], P(None, 'tp')
- output 8: float32 [2048, 5504], P(None, 'tp')
- output 9: float32 [5504, 2048], P('tp')
- output 10: float32 [2048], replicated
- output 11: float32 [2048], replicated
All inputs are finite; a program needn't handle non-finite values.
Results may differ from the reference program's by a relative error of at most 0.0147216.
Values are sent between devices in bfloat16 or wider.
A program may use at most 1 GiB of HBM per device.

```python
import math
import jax
import jax.numpy as jnp
from jax import lax

VOCAB = 32000
MODEL_DIM = 2048
HEADS = 16
KV_HEADS = 16
HEAD_DIM = 128
FFN_DIM = 5504
TOK_BLOCK = 512
CP_SIZE = 2

TOKENS = 2 * CP_SIZE * TOK_BLOCK
GROUP = HEADS // KV_HEADS
HOT_COUNT = 2 ** 5
NORM_EPS = 1e-5
SCORE_SCALE = HEAD_DIM ** -0.5
NEG_BIG = -1e30


def slot_sequence():
    slot = jnp.arange(TOKENS)
    shard = slot // (2 * TOK_BLOCK)
    within = slot % (2 * TOK_BLOCK)
    block_no = jnp.where(within < TOK_BLOCK, shard, 2 * CP_SIZE - 1 - shard)
    return block_no * TOK_BLOCK + within % TOK_BLOCK


def draw_layout(key):
    keys = jax.random.split(key, 5)
    seq_pos = slot_sequence()
    cuts = jax.random.randint(keys[0], (CP_SIZE,), 1, TOKENS)
    after_cut = cuts[None, :] <= seq_pos[:, None]
    doc_id = jnp.sum(after_cut.astype(jnp.int32), axis=1)
    doc_start = jnp.max(jnp.where(after_cut, cuts[None, :], 0), axis=1)
    pos = (seq_pos - doc_start).astype(jnp.int32)
    hot_ids = jax.random.randint(keys[1], (HOT_COUNT,), 0, VOCAB // 8)
    hot_pick = jax.random.randint(keys[2], (TOKENS,), 0, HOT_COUNT)
    spread_ids = jax.random.randint(keys[3], (TOKENS,), 0, VOCAB)
    use_hot = jax.random.randint(keys[4], (TOKENS,), 0, 2)
    tokens = jnp.where(use_hot == 1, hot_ids[hot_pick], spread_ids)
    tokens = tokens.at[0].set(0).at[1].set(VOCAB - 1)
    return tokens, pos, doc_id.astype(jnp.int32)


def setup_inputs(seed: int = 0) -> dict:
    base = jax.random.key(seed)
    tokens, pos, doc_id = draw_layout(jax.random.fold_in(base, 1))
    keys = jax.random.split(jax.random.fold_in(base, 2), 14)

    def weight(which, fan_in, fan_out):
        return (jax.random.normal(keys[which], (fan_in, fan_out), jnp.float32) * fan_in ** -0.5).astype(jnp.bfloat16)

    def gain(which):
        return (1.0 + 0.25 * jax.random.normal(keys[which], (MODEL_DIM,), jnp.float32)).astype(jnp.bfloat16)

    log_theta = jax.random.uniform(keys[11], (), jnp.float32, math.log(1e4), math.log(5e5))
    exponent = jnp.arange(HEAD_DIM // 2, dtype=jnp.float32) * (2.0 / HEAD_DIM)
    jitter = jax.random.uniform(keys[12], (HEAD_DIM // 2,), jnp.float32, 0.9, 1.1)
    return {
        "tokens": tokens,
        "pos": pos,
        "doc_id": doc_id,
        "dy": jax.random.normal(keys[0], (TOKENS, MODEL_DIM), jnp.float32).astype(jnp.bfloat16),
        "table": jax.random.normal(keys[1], (VOCAB, MODEL_DIM), jnp.float32).astype(jnp.bfloat16),
        "w_q": weight(2, MODEL_DIM, HEADS * HEAD_DIM),
        "w_k": weight(3, MODEL_DIM, KV_HEADS * HEAD_DIM),
        "w_v": weight(4, MODEL_DIM, KV_HEADS * HEAD_DIM),
        "w_o": weight(5, HEADS * HEAD_DIM, MODEL_DIM),
        "w_gate": weight(6, MODEL_DIM, FFN_DIM),
        "w_up": weight(7, MODEL_DIM, FFN_DIM),
        "w_down": weight(8, FFN_DIM, MODEL_DIM),
        "gain_one": gain(9),
        "gain_two": gain(10),
        "inv_freq": jnp.exp(-log_theta * exponent) * jitter,
    }


def to_bf16(feats):
    return feats.astype(jnp.bfloat16).astype(jnp.float32)


def rms_norm(feats, gain_vec):
    return feats * lax.rsqrt(jnp.mean(feats * feats, axis=-1, keepdims=True) + NORM_EPS) * gain_vec


def rotate(tensor_in, cosine, sine):
    half = tensor_in.shape[-1] // 2
    first = tensor_in[..., :half]
    second = tensor_in[..., half:]
    return jnp.concatenate([first * cosine - second * sine, second * cosine + first * sine], axis=-1)


def forward_pass(params, tokens, pos, doc_id, inv_freq):
    table, w_q, w_k, w_v, w_o, w_gate, w_up, w_down, gain_one, gain_two = params
    embed = jnp.take(table, tokens, axis=0)
    act_one = to_bf16(rms_norm(embed, gain_one))
    angle = pos.astype(jnp.float32)[:, None, None] * inv_freq
    cosine = jnp.cos(angle)
    sine = jnp.sin(angle)
    query = jnp.dot(act_one, w_q, preferred_element_type=jnp.float32).reshape(TOKENS, HEADS, HEAD_DIM)
    query = to_bf16(rotate(query, cosine, sine)).reshape(2 * CP_SIZE, TOK_BLOCK, KV_HEADS, GROUP, HEAD_DIM)
    key_all = jnp.dot(act_one, w_k, preferred_element_type=jnp.float32).reshape(TOKENS, KV_HEADS, HEAD_DIM)
    key_all = to_bf16(rotate(key_all, cosine, sine))
    value_all = to_bf16(jnp.dot(act_one, w_v, preferred_element_type=jnp.float32)).reshape(TOKENS, KV_HEADS, HEAD_DIM)
    seq_pos = slot_sequence()

    def attend(block):
        query_blk, seq_blk, doc_blk = block
        scores = jnp.einsum("qkgd,skd->kgqs", query_blk, key_all) * SCORE_SCALE
        allowed = (doc_blk[:, None] == doc_id[None, :]) & (seq_pos[None, :] <= seq_blk[:, None])
        attn_prob = jax.nn.softmax(jnp.where(allowed, scores, NEG_BIG), axis=-1)
        return jnp.einsum("kgqs,skd->qkgd", to_bf16(attn_prob), value_all)

    blocks = (query, seq_pos.reshape(2 * CP_SIZE, TOK_BLOCK), doc_id.reshape(2 * CP_SIZE, TOK_BLOCK))
    attended = to_bf16(lax.map(jax.checkpoint(attend), blocks)).reshape(TOKENS, HEADS * HEAD_DIM)
    residual = embed + jnp.dot(attended, w_o, preferred_element_type=jnp.float32)
    act_two = to_bf16(rms_norm(residual, gain_two))
    gate = jnp.dot(act_two, w_gate, preferred_element_type=jnp.float32)
    hidden = to_bf16(jax.nn.silu(gate) * jnp.dot(act_two, w_up, preferred_element_type=jnp.float32))
    return residual + jnp.dot(hidden, w_down, preferred_element_type=jnp.float32)


def reference(tokens, pos, doc_id, dy, table, w_q, w_k, w_v, w_o, w_gate, w_up, w_down, gain_one, gain_two, inv_freq):
    params = tuple(weight.astype(jnp.float32) for weight in (table, w_q, w_k, w_v, w_o, w_gate, w_up, w_down, gain_one, gain_two))
    layer_out, pullback = jax.vjp(lambda *weights: forward_pass(weights, tokens, pos, doc_id, inv_freq), *params)
    grads = pullback(dy.astype(jnp.float32))
    return (layer_out.astype(jnp.bfloat16), grads[0], grads[1], grads[2], grads[3], grads[4], grads[5], grads[6], grads[7], grads[8], grads[9])
```

```python
import functools

import jax
import jax.numpy as jnp
from jax import lax
from jax.experimental import pallas as pl
from jax.experimental.pallas import tpu as pltpu
from jax.sharding import PartitionSpec as P

NORM_EPS = 1e-5
NEG_BIG = -1e30
MESH = pl.DeviceIdType.MESH
NN = (((1,), (0,)), ((), ()))
NT = (((1,), (1,)), ((), ()))
VMEM_LIMIT = 60 * 1024 * 1024
F32 = jnp.float32
BF16 = jnp.bfloat16


def rms_stats(feats):
    inv_rms = lax.rsqrt(jnp.mean(feats * feats, axis=-1, keepdims=True) + NORM_EPS)
    return feats * inv_rms, inv_rms


def rms_back(d_normed, normed, inv_rms):
    return inv_rms * (d_normed - normed * jnp.mean(d_normed * normed, axis=-1, keepdims=True))


def rotate(tensor_in, cosine, sine):
    half = tensor_in.shape[-1] // 2
    first = tensor_in[..., :half]
    second = tensor_in[..., half:]
    return jnp.concatenate([first * cosine - second * sine, second * cosine + first * sine], axis=-1)


def to_bf16(feats):
    return feats.astype(BF16).astype(F32)


def slot_sequence(slot, block_len, cp_count):
    shard = slot // (2 * block_len)
    within = slot % (2 * block_len)
    block_no = jnp.where(within < block_len, shard, 2 * cp_count - 1 - shard)
    return block_no * block_len + within % block_len


def neighbours():
    me = lax.axis_index("tp")
    return me, me + 1 - 2 * lax.rem(me, 2), lax.rem(me + 2, 4), 3 - me


def enter(peers):
    barrier = pltpu.get_barrier_semaphore()
    for peer in peers:
        pl.semaphore_signal(barrier, inc=1, device_id={"tp": peer}, device_id_type=MESH)
    pl.semaphore_wait(barrier, len(peers))


def remote(src, dst, sems, slot, peer):
    return pltpu.make_async_remote_copy(
        src_ref=src, dst_ref=dst, send_sem=sems.at[0, slot], recv_sem=sems.at[1, slot],
        device_id={"tp": peer}, device_id_type=MESH)


def sum_kernel(dims, count, has_add, *refs):
    lhs = refs[:count]
    rhs = refs[count:2 * count]
    rest = refs[2 * count:]
    out_ref, part, recv1, recv2, sems = rest
    wide = part.dtype
    block, half = part.shape[2], part.shape[3]
    me, x_peer, y_peer, diag = neighbours()
    peers = (x_peer, y_peer)
    enter(peers)

    def compute(side, owner):
        rows = pl.ds(pl.multiple_of(owner * block, block), block)
        if dims is None:
            part[side, owner] = lhs[0][rows, side * half:(side + 1) * half]
            return
        tile = 256

        def step(j, carry):
            total = None
            for left, right in zip(lhs, rhs):
                start = pl.multiple_of(side * half + j * tile, tile)
                piece = right[pl.ds(start, tile), :] if dims == NT else right[:, pl.ds(start, tile)]
                term = lax.dot_general(left[rows, :], piece, dims, preferred_element_type=F32)
                total = term if total is None else total + term
            part[side, owner, :, pl.ds(pl.multiple_of(j * tile, tile), tile)] = total
            return carry

        lax.fori_loop(0, half // tile, step, 0)

    first = []
    for k in range(2):
        for side in range(2):
            owner = diag if k == 0 else peers[side]
            compute(side, owner)
            copy = remote(part.at[side, owner], recv1.at[side, k], sems, side * 2 + k, peers[side])
            copy.start()
            first.append(copy)
    for side in range(2):
        compute(side, peers[1 - side])
    for side in range(2):
        compute(side, me)
    second = []
    for side in range(2):
        first[side].wait_recv()
        owner = peers[1 - side]
        part[side, owner] = (part[side, owner].astype(F32) + recv1[side, 0].astype(F32)).astype(wide)
        copy = remote(part.at[side, owner], recv2.at[side], sems, 4 + side, peers[1 - side])
        copy.start()
        second.append(copy)
    mine = pl.ds(pl.multiple_of(me * block, block), block)
    own = []
    for side in range(2):
        first[2 + side].wait_recv()
        second[side].wait_recv()
        total = part[side, me].astype(F32) + recv1[side, 1].astype(F32) + recv2[side].astype(F32)
        cols = slice(side * half, (side + 1) * half)
        out_ref[mine, cols] = total.astype(out_ref.dtype)
        copy = remote(out_ref.at[mine, cols], out_ref.at[mine, cols], sems, 6 + side, peers[1 - side])
        copy.start()
        own.append(copy)
    far = []
    for side in range(2):
        cols = slice(side * half, (side + 1) * half)
        copy = remote(out_ref.at[mine, cols], out_ref.at[mine, cols], sems, 8 + side, peers[side])
        copy.start()
        far.append(copy)
    for side in range(2):
        cols = slice(side * half, (side + 1) * half)
        own[side].wait_recv()
        rows = pl.ds(pl.multiple_of(peers[1 - side] * block, block), block)
        copy = remote(out_ref.at[rows, cols], out_ref.at[rows, cols], sems, 10 + side, peers[side])
        copy.start()
        far.append(copy)
    for copy in far:
        copy.wait_recv()
    for copy in first + second + own + far:
        copy.wait_send()


def tp_sum(lhs, rhs, dims, collective_id):
    span = lhs[0].shape[0]
    width = lhs[0].shape[1] if dims is None else rhs[0].shape[0 if dims == NT else 1]
    block, half = span // 4, width // 2
    wide = BF16 if dims is None else F32
    count = len(lhs)
    vmem = pl.BlockSpec(memory_space=pltpu.VMEM)
    return pl.pallas_call(
        functools.partial(sum_kernel, dims, count, False) if rhs else functools.partial(copy_sum_kernel),
        out_shape=jax.ShapeDtypeStruct((span, width), BF16),
        in_specs=[vmem] * (count + len(rhs)),
        out_specs=vmem,
        scratch_shapes=[
            pltpu.VMEM((2, 4, block, half), wide),
            pltpu.VMEM((2, 2, block, half), wide),
            pltpu.VMEM((2, block, half), wide),
            pltpu.SemaphoreType.DMA((2, 12)),
        ],
        compiler_params=pltpu.CompilerParams(
            collective_id=collective_id, has_side_effects=True, vmem_limit_bytes=VMEM_LIMIT),
        name=f"tp_sum_{collective_id}",
    )(*lhs, *rhs)


def copy_sum_kernel(*refs):
    sum_kernel(None, 1, False, refs[0], None, *refs[1:])


def out_proj_kernel(att_ref, w_ref, embed_ref, res_ref, slots, sems):
    me, x_peer, y_peer, diag = neighbours()
    peers = (x_peer, y_peer)
    enter(peers)
    width = att_ref.shape[1]
    half = att_ref.shape[0] // 2
    sides = [pl.ds(0, half), pl.ds(half, half)]

    def multiply(block, owner, initial):
        tile = 256

        def step(j, carry):
            cols = pl.ds(pl.multiple_of(j * tile, tile), tile)
            rows = pl.ds(pl.multiple_of(owner * width, width), width)
            term = jnp.dot(block[...], w_ref[rows, cols], preferred_element_type=F32)
            if initial:
                res_ref[:, cols] = term
            else:
                res_ref[:, cols] = res_ref[:, cols] + term
            return carry

        lax.fori_loop(0, w_ref.shape[1] // tile, step, 0)

    near = []
    for side in range(2):
        copy = remote(att_ref.at[sides[side]], slots.at[me, sides[side]], sems, side, peers[side])
        copy.start()
        near.append(copy)
    far = []
    for side in range(2):
        copy = remote(att_ref.at[sides[side]], slots.at[me, sides[side]], sems, 2 + side, peers[1 - side])
        copy.start()
        far.append(copy)
    multiply(att_ref, me, True)
    last = []
    for side in range(2):
        near[side].wait_recv()
        owner = peers[side]
        copy = remote(slots.at[owner, sides[side]], slots.at[owner, sides[side]], sems, 4 + side, peers[1 - side])
        copy.start()
        last.append(copy)
    for side in range(2):
        far[side].wait_recv()
    for side in range(2):
        multiply(slots.at[peers[side]], peers[side], False)
    for side in range(2):
        last[side].wait_recv()
    multiply(slots.at[diag], diag, False)
    tile = 256

    def add(j, carry):
        cols = pl.ds(pl.multiple_of(j * tile, tile), tile)
        res_ref[:, cols] = embed_ref[:, cols].astype(F32) + res_ref[:, cols]
        return carry

    lax.fori_loop(0, w_ref.shape[1] // tile, add, 0)
    for copy in near + far + last:
        copy.wait_send()


def out_proj(attended, w_all, embed, collective_id):
    span, width = attended.shape
    vmem = pl.BlockSpec(memory_space=pltpu.VMEM)
    return pl.pallas_call(
        out_proj_kernel,
        out_shape=jax.ShapeDtypeStruct(embed.shape, F32),
        in_specs=[vmem] * 3,
        out_specs=vmem,
        scratch_shapes=[pltpu.VMEM((4, span, width), BF16), pltpu.SemaphoreType.DMA((2, 6))],
        compiler_params=pltpu.CompilerParams(
            collective_id=collective_id, has_side_effects=True, vmem_limit_bytes=VMEM_LIMIT),
        name="out_proj",
    )(attended, w_all, embed)


def solution(mesh):
    cp_count = mesh.shape["cp"]

    def device_step(tokens, pos, doc_id, dy, table, w_q, w_k, w_v, w_o, w_gate, w_up, w_down, gain_one, gain_two, inv_freq):
        span = tokens.shape[0]
        total = span * cp_count
        rows = table.shape[0]
        head_dim = 2 * inv_freq.shape[0]
        kv_local = w_k.shape[1] // head_dim
        q_local = w_q.shape[1] // head_dim
        group = q_local // kv_local
        scale = head_dim ** -0.5
        tp_rank = lax.axis_index("tp")
        cp_rank = lax.axis_index("cp")
        gain_a = gain_one.astype(F32)
        gain_b = gain_two.astype(F32)
        swap = [(0, 1), (1, 0)]

        local_ids = tokens - tp_rank * rows
        owned = (local_ids >= 0) & (local_ids < rows)
        safe_ids = jnp.where(owned, local_ids, 0)
        picked = jnp.where(owned[:, None], jnp.take(table, safe_ids, axis=0), jnp.zeros((), BF16))
        embed_b = tp_sum([picked], [], None, 0)
        embed = embed_b.astype(F32)

        normed_a, inv_a = rms_stats(embed)
        act_a = (normed_a * gain_a).astype(BF16)
        angle = pos.astype(F32)[:, None, None] * inv_freq
        cosine = jnp.cos(angle)
        sine = jnp.sin(angle)
        query = jnp.dot(act_a, w_q, preferred_element_type=F32).reshape(span, q_local, head_dim)
        query = rotate(query, cosine, sine).astype(BF16).reshape(span, kv_local, group, head_dim)
        key_loc = jnp.dot(act_a, w_k, preferred_element_type=F32).reshape(span, kv_local, head_dim)
        key_loc = rotate(key_loc, cosine, sine).astype(BF16)
        value_loc = jnp.dot(act_a, w_v, preferred_element_type=F32).astype(BF16).reshape(span, kv_local, head_dim)

        key_all = lax.all_gather(key_loc, "cp", axis=0, tiled=True)
        value_all = lax.all_gather(value_loc, "cp", axis=0, tiled=True)
        w_tied, key_all, value_all = lax.optimization_barrier((w_o, key_all, value_all))
        w_o_all = lax.all_gather(w_tied, "tp", axis=0, tiled=True)
        doc_all = lax.all_gather(doc_id, "cp", axis=0, tiled=True)
        q_seq = slot_sequence(cp_rank * span + jnp.arange(span), span // 2, cp_count)
        k_seq = slot_sequence(jnp.arange(total), span // 2, cp_count)
        allowed = (doc_id[:, None] == doc_all[None, :]) & (k_seq[None, :] <= q_seq[:, None])

        scores = jnp.einsum("qkgd,skd->kgqs", query, key_all, preferred_element_type=F32) * scale
        attn_prob = jax.nn.softmax(jnp.where(allowed, scores, NEG_BIG), axis=-1)
        prob_b = attn_prob.astype(BF16)
        attended = jnp.einsum("kgqs,skd->qkgd", prob_b, value_all, preferred_element_type=F32)
        attended = attended.astype(BF16).reshape(span, q_local * head_dim)
        residual = out_proj(attended, w_o_all, embed_b, 1)
        normed_b, inv_b = rms_stats(residual)
        act_b = (normed_b * gain_b).astype(BF16)
        gate = jnp.dot(act_b, w_gate, preferred_element_type=F32)
        up_val = jnp.dot(act_b, w_up, preferred_element_type=F32)
        gate_sig = jax.nn.sigmoid(gate)
        hidden = (gate * gate_sig * up_val).astype(BF16)
        d_hidden = to_bf16(jnp.einsum("td,fd->tf", dy, w_down, preferred_element_type=F32))
        d_gate = (d_hidden * up_val * gate_sig * (1.0 + gate * (1.0 - gate_sig))).astype(BF16)
        d_up = (d_hidden * gate * gate_sig).astype(BF16)
        d_act_b = tp_sum([d_gate, d_up], [w_gate, w_up], NT, 2)

        hidden_late, d_act_b = lax.optimization_barrier((hidden, d_act_b))
        out_part = jnp.dot(hidden_late, w_down, preferred_element_type=F32)
        out_mine = lax.psum_scatter(out_part, "tp", scatter_dimension=0, tiled=True)
        res_mine = lax.dynamic_slice_in_dim(residual, tp_rank * (span // 4), span // 4, axis=0)
        layer_out = lax.all_gather((out_mine + res_mine).astype(BF16), "tp", axis=0, tiled=True)

        grad_down = jnp.einsum("tf,td->fd", hidden_late, dy, preferred_element_type=F32)
        grad_gate = jnp.einsum("td,tf->df", act_b, d_gate, preferred_element_type=F32)
        grad_up = jnp.einsum("td,tf->df", act_b, d_up, preferred_element_type=F32)
        d_act_b = d_act_b.astype(F32)
        grad_gain_b = jnp.sum(d_act_b * normed_b, axis=0)
        d_resid = dy.astype(F32) + rms_back(d_act_b * gain_b, normed_b, inv_b)
        d_resid_b = d_resid.astype(BF16)
        grad_out = jnp.einsum("tc,td->cd", attended, d_resid_b, preferred_element_type=F32)
        d_att = jnp.einsum("td,cd->tc", d_resid_b, w_o, preferred_element_type=F32)
        d_att = d_att.astype(BF16).reshape(span, kv_local, group, head_dim)
        d_prob = to_bf16(jnp.einsum("qkgd,skd->kgqs", d_att, value_all, preferred_element_type=F32))
        d_scores = attn_prob * (d_prob - jnp.sum(attn_prob * d_prob, axis=-1, keepdims=True))
        d_scores = (d_scores * scale).astype(BF16)
        d_query = jnp.einsum("kgqs,skd->qkgd", d_scores, key_all, preferred_element_type=F32)
        d_key_all = jnp.einsum("kgqs,qkgd->skd", d_scores, query, preferred_element_type=F32)
        d_value_all = jnp.einsum("kgqs,qkgd->skd", prob_b, d_att, preferred_element_type=F32)
        d_key = lax.psum_scatter(d_key_all, "cp", scatter_dimension=0, tiled=True)
        d_value = lax.psum_scatter(d_value_all, "cp", scatter_dimension=0, tiled=True)
        d_q_pre = rotate(to_bf16(d_query).reshape(span, q_local, head_dim), cosine, -sine)
        d_q_pre = d_q_pre.astype(BF16).reshape(span, q_local * head_dim)
        d_k_pre = rotate(to_bf16(d_key), cosine, -sine).astype(BF16).reshape(span, kv_local * head_dim)
        d_v_pre = d_value.astype(BF16).reshape(span, kv_local * head_dim)
        mlp_grads = lax.psum((grad_gate, grad_up, grad_down), "cp")
        d_act_a = tp_sum([d_q_pre, d_k_pre, d_v_pre], [w_q, w_k, w_v], NT, 3)
        grad_q = jnp.einsum("td,tc->dc", act_a, d_q_pre, preferred_element_type=F32)
        grad_k = jnp.einsum("td,tc->dc", act_a, d_k_pre, preferred_element_type=F32)
        grad_v = jnp.einsum("td,tc->dc", act_a, d_v_pre, preferred_element_type=F32)
        d_act_a = d_act_a.astype(F32)
        grad_gain_a = jnp.sum(d_act_a * normed_a, axis=0)
        d_embed = d_resid + rms_back(d_act_a * gain_a, normed_a, inv_a)
        d_embed_other = lax.ppermute(d_embed, "cp", swap)
        tokens_other = lax.ppermute(tokens, "cp", swap)
        even = cp_rank == 0
        all_ids = jnp.where(even, jnp.concatenate([tokens, tokens_other]), jnp.concatenate([tokens_other, tokens])) - tp_rank * rows
        all_grads = jnp.where(even, jnp.concatenate([d_embed, d_embed_other]), jnp.concatenate([d_embed_other, d_embed]))
        all_ids = jnp.where((all_ids >= 0) & (all_ids < rows), all_ids, rows)
        grad_table = jax.ops.segment_sum(all_grads, all_ids, num_segments=rows)
        att_grads = lax.psum((grad_q, grad_k, grad_v, grad_out), "cp")
        gains = lax.psum((grad_gain_a, grad_gain_b), "cp")
        grad_gate, grad_up, grad_down = mlp_grads
        return (layer_out, grad_table) + tuple(att_grads) + (grad_gate, grad_up, grad_down) + tuple(gains)

    col_spec = P(None, "tp")
    row_spec = P("tp", None)
    tok_spec = P("cp")
    rep_spec = P(None)
    in_specs = (tok_spec, tok_spec, tok_spec, P("cp", None), row_spec, col_spec, col_spec, col_spec, row_spec, col_spec, col_spec, row_spec, rep_spec, rep_spec, rep_spec)
    out_specs = (P("cp", None), row_spec, col_spec, col_spec, col_spec, row_spec, col_spec, col_spec, row_spec, rep_spec, rep_spec)
    return jax.shard_map(device_step, mesh=mesh, in_specs=in_specs, out_specs=out_specs, check_vma=False)
```

```python
import functools

import jax
import jax.numpy as jnp
from jax import lax
from jax.experimental import pallas as pl
from jax.experimental.pallas import tpu as pltpu
from jax.sharding import PartitionSpec as P

NORM_EPS = 1e-5
NEG_BIG = -1e30
MESH = pl.DeviceIdType.MESH
NN = (((1,), (0,)), ((), ()))
NT = (((1,), (1,)), ((), ()))
VMEM_LIMIT = 60 * 1024 * 1024
F32 = jnp.float32
BF16 = jnp.bfloat16


def rms_stats(feats):
    inv_rms = lax.rsqrt(jnp.mean(feats * feats, axis=-1, keepdims=True) + NORM_EPS)
    return feats * inv_rms, inv_rms


def rms_back(d_normed, normed, inv_rms):
    return inv_rms * (d_normed - normed * jnp.mean(d_normed * normed, axis=-1, keepdims=True))


def to_bf16(feats):
    return feats.astype(BF16).astype(F32)


def neighbours():
    me = lax.axis_index("tp")
    return me, me + 1 - 2 * lax.rem(me, 2), lax.rem(me + 2, 4), 3 - me


def enter(peers):
    barrier = pltpu.get_barrier_semaphore()
    for peer in peers:
        pl.semaphore_signal(barrier, inc=1, device_id={"tp": peer}, device_id_type=MESH)
    pl.semaphore_wait(barrier, len(peers))


def remote(src, dst, sems, slot, peer):
    return pltpu.make_async_remote_copy(
        src_ref=src, dst_ref=dst, send_sem=sems.at[0, slot], recv_sem=sems.at[1, slot],
        device_id={"tp": peer}, device_id_type=MESH)


def tp_exchange(compute, done, out_ref, part, recv1, recv2, sems):
    wide = part.dtype
    block, half = part.shape[2], part.shape[3]
    me, x_peer, y_peer, diag = neighbours()
    peers = (x_peer, y_peer)

    first = []
    for k in range(2):
        for side in range(2):
            owner = diag if k == 0 else peers[side]
            compute(side, owner)
            copy = remote(part.at[side, owner], recv1.at[side, k], sems, side * 2 + k, peers[side])
            copy.start()
            first.append(copy)
    for side in range(2):
        compute(side, peers[1 - side])
    for side in range(2):
        compute(side, me)
    second = []
    for side in range(2):
        first[side].wait_recv()
        owner = peers[1 - side]
        part[side, owner] = (part[side, owner].astype(F32) + recv1[side, 0].astype(F32)).astype(wide)
        copy = remote(part.at[side, owner], recv2.at[side], sems, 4 + side, peers[1 - side])
        copy.start()
        second.append(copy)
    mine = pl.ds(pl.multiple_of(me * block, block), block)
    sides = [slice(side * half, (side + 1) * half) for side in range(2)]
    own = []
    for side in range(2):
        first[2 + side].wait_recv()
        second[side].wait_recv()
        total = part[side, me].astype(F32) + recv1[side, 1].astype(F32) + recv2[side].astype(F32)
        out_ref[mine, sides[side]] = total.astype(out_ref.dtype)
        copy = remote(out_ref.at[mine, sides[side]], out_ref.at[mine, sides[side]], sems, 6 + side, peers[1 - side])
        copy.start()
        own.append(copy)
    far = []
    for side in range(2):
        copy = remote(out_ref.at[mine, sides[side]], out_ref.at[mine, sides[side]], sems, 8 + side, peers[side])
        copy.start()
        far.append(copy)
    done(me)
    for side in range(2):
        own[side].wait_recv()
        rows = pl.ds(pl.multiple_of(peers[1 - side] * block, block), block)
        copy = remote(out_ref.at[rows, sides[side]], out_ref.at[rows, sides[side]], sems, 10 + side, peers[side])
        copy.start()
        far.append(copy)
    for side in range(2):
        far[side].wait_recv()
    done(x_peer)
    done(y_peer)
    for side in range(2):
        far[2 + side].wait_recv()
    done(diag)
    for copy in first + second + own + far:
        copy.wait_send()


def exchange_scratch(span, width, wide):
    block, half = span // 4, width // 2
    return [
        pltpu.VMEM((2, 4, block, half), wide),
        pltpu.VMEM((2, 2, block, half), wide),
        pltpu.VMEM((2, block, half), wide),
        pltpu.SemaphoreType.DMA((2, 12)),
    ]


EXCHANGE_COST = pl.CostEstimate(flops=10**11, bytes_accessed=10**8, transcendentals=0)


def comm_params(collective_id):
    return pltpu.CompilerParams(collective_id=collective_id, has_side_effects=True, vmem_limit_bytes=VMEM_LIMIT)


VMEM_SPEC = pl.BlockSpec(memory_space=pltpu.VMEM)


def product_into(part, lhs, rhs, dims):
    block, half = part.shape[2], part.shape[3]
    tile = 256

    def compute(side, owner):
        rows = pl.ds(pl.multiple_of(owner * block, block), block)

        def step(j, carry):
            total = None
            for left, right in zip(lhs, rhs):
                start = pl.multiple_of(side * half + j * tile, tile)
                piece = right[pl.ds(start, tile), :] if dims == NT else right[:, pl.ds(start, tile)]
                term = lax.dot_general(left[rows, :], piece, dims, preferred_element_type=F32)
                total = term if total is None else total + term
            part[side, owner, :, pl.ds(pl.multiple_of(j * tile, tile), tile)] = total
            return carry

        lax.fori_loop(0, half // tile, step, 0)

    return compute


def inverse_root(value):
    guess = lax.rsqrt(value)
    return guess * (1.5 - 0.5 * value * guess * guess)


def turn(feats, cosine, sine):
    return feats * cosine + pltpu.roll(feats, feats.shape[-1] // 2, 1) * sine


def embed_kernel(picked, gain, w_q, w_k, w_v, cosine, sine, embed, act, q_ref, k_ref, v_ref, part, recv1, recv2, sems, kv_sems):
    block, half = part.shape[2], part.shape[3]
    span = picked.shape[0]
    head = cosine.shape[1]
    me, x_peer, y_peer, diag = neighbours()
    cp = lax.axis_index("cp")
    barrier = pltpu.get_barrier_semaphore()
    for peer in ({"tp": x_peer}, {"tp": y_peer}, {"cp": 1 - cp}):
        pl.semaphore_signal(barrier, inc=1, device_id=peer, device_id_type=MESH)
    pl.semaphore_wait(barrier, 3)
    sent = []

    def compute(side, owner):
        rows = pl.ds(pl.multiple_of(owner * block, block), block)
        part[side, owner] = picked[rows, side * half:(side + 1) * half]

    def done(owner):
        rows = pl.ds(pl.multiple_of(owner * block, block), block)
        slots = pl.ds(pl.multiple_of(cp * span + owner * block, block), block)
        feats = embed[rows, :].astype(F32)
        inv_rms = inverse_root(jnp.mean(feats * feats, axis=-1, keepdims=True) + NORM_EPS)
        act[rows, :] = (feats * inv_rms * gain[...]).astype(BF16)

        def step(j, carry):
            cols = pl.ds(pl.multiple_of(j * head, head), head)
            left = act[rows, :]
            query = jnp.dot(left, w_q[:, cols], preferred_element_type=F32)
            q_ref[rows, cols] = turn(query, cosine[rows, :], sine[rows, :]).astype(BF16)
            key = jnp.dot(left, w_k[:, cols], preferred_element_type=F32)
            k_ref[slots, cols] = turn(key, cosine[rows, :], sine[rows, :]).astype(BF16)
            v_ref[slots, cols] = jnp.dot(left, w_v[:, cols], preferred_element_type=F32).astype(BF16)
            return carry

        lax.fori_loop(0, w_q.shape[1] // head, step, 0)
        for ref in (k_ref, v_ref):
            slot = len(sent)
            copy = pltpu.make_async_remote_copy(
                src_ref=ref.at[slots], dst_ref=ref.at[slots], send_sem=kv_sems.at[0, slot], recv_sem=kv_sems.at[1, slot],
                device_id={"cp": 1 - cp}, device_id_type=MESH)
            copy.start()
            sent.append(copy)

    tp_exchange(compute, done, embed, part, recv1, recv2, sems)
    for copy in sent:
        copy.wait_recv()
    for copy in sent:
        copy.wait_send()


def embed_qkv(picked, gain, w_q, w_k, w_v, cosine, sine, cp_count, collective_id):
    span, width = picked.shape
    cols = w_q.shape[1]
    return pl.pallas_call(
        embed_kernel,
        out_shape=[jax.ShapeDtypeStruct(shape, BF16) for shape in (
            (span, width), (span, width), (span, cols), (span * cp_count, cols), (span * cp_count, cols))],
        in_specs=[VMEM_SPEC] * 7,
        out_specs=[VMEM_SPEC] * 5,
        scratch_shapes=exchange_scratch(span, width, BF16) + [pltpu.SemaphoreType.DMA((2, 8))],
        compiler_params=comm_params(collective_id),
        cost_estimate=EXCHANGE_COST,
        name="embed_qkv",
    )(picked, gain, w_q, w_k, w_v, cosine, sine)


def grad_b_kernel(d_gate, d_up, w_gate, w_up, out, part, recv1, recv2, sems):
    enter(neighbours()[1:3])
    tp_exchange(product_into(part, (d_gate, d_up), (w_gate, w_up), NN), lambda owner: None, out, part, recv1, recv2, sems)


def grad_b(d_gate, d_up, w_gate_t, w_up_t, collective_id):
    span, width = d_gate.shape[0], w_gate_t.shape[1]
    return pl.pallas_call(
        grad_b_kernel,
        out_shape=jax.ShapeDtypeStruct((span, width), BF16),
        in_specs=[VMEM_SPEC] * 4,
        out_specs=VMEM_SPEC,
        scratch_shapes=exchange_scratch(span, width, F32),
        compiler_params=comm_params(collective_id),
        cost_estimate=EXCHANGE_COST,
        name="grad_b",
    )(d_gate, d_up, w_gate_t, w_up_t)


def grad_a_kernel(
    d_q, d_k_all, d_v_all, w_q, w_k, w_v, cosine, sine, embed, gain, d_resid,
    d_embed, grad_gain, d_k, d_v, out, resid, recv_k, recv_v, part, recv1, recv2, sems, kv_sems, row_sems):
    span = d_q.shape[0]
    block = part.shape[2]
    head = cosine.shape[1]
    me, x_peer, y_peer, diag = neighbours()
    cp = lax.axis_index("cp")
    barrier = pltpu.get_barrier_semaphore()
    for peer in ({"tp": x_peer}, {"tp": y_peer}, {"cp": 1 - cp}):
        pl.semaphore_signal(barrier, inc=1, device_id=peer, device_id_type=MESH)
    pl.semaphore_wait(barrier, 3)
    load = pltpu.make_async_copy(d_resid, resid, row_sems.at[0, 0])
    load.start()
    order = (diag, x_peer, y_peer, me)
    copies = []
    for place, owner in enumerate(order):
        rows = pl.ds(pl.multiple_of(owner * block, block), block)
        theirs = pl.ds(pl.multiple_of((1 - cp) * span + owner * block, block), block)
        for which, (source, target) in enumerate(((d_k_all, recv_k), (d_v_all, recv_v))):
            slot = 2 * place + which
            copy = pltpu.make_async_remote_copy(
                src_ref=source.at[theirs], dst_ref=target.at[rows], send_sem=kv_sems.at[0, slot], recv_sem=kv_sems.at[1, slot],
                device_id={"cp": 1 - cp}, device_id_type=MESH)
            copy.start()
            copies.append(copy)
    product = product_into(part, (d_q, d_k, d_v), (w_q, w_k, w_v), NT)
    ready = []

    def prepare(place):
        owner = order[place]
        copies[2 * place].wait_recv()
        copies[2 * place + 1].wait_recv()
        rows = pl.ds(pl.multiple_of(owner * block, block), block)
        ours = pl.ds(pl.multiple_of(cp * span + owner * block, block), block)

        def step(j, carry):
            cols = pl.ds(pl.multiple_of(j * head, head), head)
            total = (d_k_all[ours, cols] + recv_k[rows, cols]).astype(BF16).astype(F32)
            d_k[rows, cols] = turn(total, cosine[rows, :], -sine[rows, :]).astype(BF16)
            d_v[rows, cols] = (d_v_all[ours, cols] + recv_v[rows, cols]).astype(BF16)
            return carry

        lax.fori_loop(0, d_q.shape[1] // head, step, 0)
        ready.append(place)

    calls = []

    def compute(side, owner):
        turn_no = len(calls)
        calls.append(side)
        if turn_no == 0:
            prepare(0)
        elif turn_no == 2:
            prepare(1)
        elif turn_no == 3:
            prepare(2)
        elif turn_no == 6:
            prepare(3)
        product(side, owner)

    grad_gain[...] = jnp.zeros_like(grad_gain)
    local, shared = [], []

    def done(owner):
        if not local:
            load.wait()
        rows = pl.ds(pl.multiple_of(owner * block, block), block)
        slots = pl.ds(pl.multiple_of(cp * span + owner * block, block), block)
        feats = embed[rows, :].astype(F32)
        inv_rms = inverse_root(jnp.mean(feats * feats, axis=-1, keepdims=True) + NORM_EPS)
        normed = feats * inv_rms
        d_act = out[rows, :].astype(F32)
        grad_gain[...] = grad_gain[...] + jnp.sum(d_act * normed, axis=0, keepdims=True)
        resid[rows, :] = resid[rows, :] + rms_back(d_act * gain[...], normed, inv_rms)
        slot = 1 + len(local)
        copy = pltpu.make_async_copy(resid.at[rows], d_embed.at[slots], row_sems.at[0, slot])
        copy.start()
        local.append(copy)
        copy = pltpu.make_async_remote_copy(
            src_ref=resid.at[rows], dst_ref=d_embed.at[slots], send_sem=row_sems.at[1, slot], recv_sem=row_sems.at[2, slot],
            device_id={"cp": 1 - cp}, device_id_type=MESH)
        copy.start()
        shared.append(copy)

    tp_exchange(compute, done, out, part, recv1, recv2, sems)
    for copy in local:
        copy.wait()
    for copy in shared:
        copy.wait_recv()
    for copy in copies + shared:
        copy.wait_send()


def grad_a(d_q, d_k_all, d_v_all, w_q, w_k, w_v, cosine, sine, embed, gain, d_resid, cp_count, collective_id):
    span, width = d_q.shape[0], w_q.shape[0]
    cols = d_q.shape[1]
    hbm = pl.BlockSpec(memory_space=pl.ANY)
    return pl.pallas_call(
        grad_a_kernel,
        out_shape=[
            jax.ShapeDtypeStruct((span * cp_count, width), F32), jax.ShapeDtypeStruct((1, width), F32),
            jax.ShapeDtypeStruct((span, cols), BF16), jax.ShapeDtypeStruct((span, cols), BF16)],
        in_specs=[VMEM_SPEC] * 10 + [hbm],
        out_specs=[hbm] + [VMEM_SPEC] * 3,
        scratch_shapes=[pltpu.VMEM((span, width), BF16), pltpu.VMEM((span, width), F32)] + [pltpu.VMEM((span, cols), F32)] * 2
        + exchange_scratch(span, width, F32) + [pltpu.SemaphoreType.DMA((2, 8)), pltpu.SemaphoreType.DMA((3, 5))],
        compiler_params=comm_params(collective_id),
        cost_estimate=EXCHANGE_COST,
        name="grad_a",
    )(d_q, d_k_all, d_v_all, w_q, w_k, w_v, cosine, sine, embed, gain, d_resid)


Q_TILE = 256


def key_row(chunk, size):
    return pl.multiple_of(jnp.where(chunk < 2, 2 * chunk, 7 - 2 * chunk) * size, size)


def query_plan(i, size, pos_smem):
    cp = lax.axis_index("cp")
    per_block = size // Q_TILE
    seq_block = jnp.where(i < per_block, cp, 3 - cp)
    start = seq_block * size + lax.rem(i, per_block) * Q_TILE
    low = jnp.maximum(start - pos_smem[i * Q_TILE], 0) // size
    return start, low, seq_block + 1


def distance(size):
    return lax.broadcasted_iota(jnp.int32, (Q_TILE, size), 0) - lax.broadcasted_iota(jnp.int32, (Q_TILE, size), 1)


def attend_kernel(pos_smem, q_ref, k_ref, v_ref, pos_ref, o_ref, lse_ref, held):
    size = held.shape[2]
    head = q_ref.shape[1]
    scale = head ** -0.5

    def block(i, carry):
        start, low, high = query_plan(i, size, pos_smem)
        rows = pl.ds(pl.multiple_of(i * Q_TILE, Q_TILE), Q_TILE)
        query = q_ref[rows, :]
        back = pos_ref[rows, :]

        def score(c, top):
            keys = k_ref[pl.ds(key_row(c, size), size), :]
            scores = lax.dot_general(query, keys, NT, preferred_element_type=F32) * scale
            gap = distance(size) + (start - c * size)
            scores = jnp.where((gap >= 0) & (gap <= back), scores, NEG_BIG)
            held[c] = scores
            return jnp.maximum(top, jnp.max(scores, axis=1, keepdims=True))

        top = lax.fori_loop(low, high, score, jnp.full((Q_TILE, 1), NEG_BIG, F32))

        def expo(c, total):
            prob = jnp.exp(held[c] - top)
            held[c] = prob
            return total + jnp.sum(prob, axis=1, keepdims=True)

        total = lax.fori_loop(low, high, expo, jnp.zeros((Q_TILE, 1), F32))
        share = 1.0 / total

        def gather(c, acc):
            prob = (held[c] * share).astype(BF16)
            values = v_ref[pl.ds(key_row(c, size), size), :]
            return acc + jnp.dot(prob, values, preferred_element_type=F32)

        acc = lax.fori_loop(low, high, gather, jnp.zeros((Q_TILE, head), F32))
        o_ref[rows, :] = acc.astype(BF16)
        lse_ref[rows, :] = jnp.broadcast_to(top + jnp.log(total), (Q_TILE, head))
        return carry

    lax.fori_loop(0, q_ref.shape[0] // Q_TILE, block, 0)


def attend_back_kernel(pos_smem, q_ref, k_ref, v_ref, do_ref, lse_ref, pos_ref, cosine, sine, dq_ref, dk_ref, dv_ref, held_p, held_d):
    size = held_p.shape[2]
    head = q_ref.shape[1]
    scale = head ** -0.5
    dk_ref[...] = jnp.zeros_like(dk_ref)
    dv_ref[...] = jnp.zeros_like(dv_ref)
    over_rows = (((0,), (0,)), ((), ()))

    def block(i, carry):
        start, low, high = query_plan(i, size, pos_smem)
        rows = pl.ds(pl.multiple_of(i * Q_TILE, Q_TILE), Q_TILE)
        query = q_ref[rows, :]
        d_out = do_ref[rows, :]
        lse = lse_ref[rows, :][:, :1]
        back = pos_ref[rows, :]

        def probs(c, total):
            place = pl.ds(key_row(c, size), size)
            scores = lax.dot_general(query, k_ref[place, :], NT, preferred_element_type=F32) * scale
            gap = distance(size) + (start - c * size)
            prob = jnp.where((gap >= 0) & (gap <= back), jnp.exp(scores - lse), 0.0)
            d_prob = to_bf16(lax.dot_general(d_out, v_ref[place, :], NT, preferred_element_type=F32))
            held_p[c] = prob
            held_d[c] = d_prob
            return total + jnp.sum(prob * d_prob, axis=1, keepdims=True)

        mean = lax.fori_loop(low, high, probs, jnp.zeros((Q_TILE, 1), F32))

        def grads(c, acc):
            place = pl.ds(key_row(c, size), size)
            prob = held_p[c]
            d_score = (prob * (held_d[c] - mean) * scale).astype(BF16)
            dk_ref[place, :] = dk_ref[place, :] + lax.dot_general(d_score, query, over_rows, preferred_element_type=F32)
            dv_ref[place, :] = dv_ref[place, :] + lax.dot_general(prob.astype(BF16), d_out, over_rows, preferred_element_type=F32)
            return acc + jnp.dot(d_score, k_ref[place, :], preferred_element_type=F32)

        d_query = lax.fori_loop(low, high, grads, jnp.zeros((Q_TILE, head), F32))
        dq_ref[rows, :] = turn(to_bf16(d_query), cosine[rows, :], -sine[rows, :]).astype(BF16)
        return carry

    lax.fori_loop(0, q_ref.shape[0] // Q_TILE, block, 0)


def attention(query, key_all, value_all, pos, head):
    span, cols = query.shape
    total = key_all.shape[0]
    size = total // 4
    own = pl.BlockSpec((span, head), lambda h, *_: (0, h))
    full = pl.BlockSpec((total, head), lambda h, *_: (0, h))
    pos_spec = pl.BlockSpec((span, 1), lambda h, *_: (0, 0))
    flops = 4 * span * total * cols
    return pl.pallas_call(
        attend_kernel,
        grid_spec=pltpu.PrefetchScalarGridSpec(
            num_scalar_prefetch=1, grid=(cols // head,), in_specs=[own, full, full, pos_spec], out_specs=[own, own],
            scratch_shapes=[pltpu.VMEM((4, Q_TILE, size), F32)]),
        out_shape=[jax.ShapeDtypeStruct((span, cols), BF16), jax.ShapeDtypeStruct((span, cols), F32)],
        cost_estimate=pl.CostEstimate(flops=flops, bytes_accessed=8 * total * cols, transcendentals=0),
        compiler_params=pltpu.CompilerParams(vmem_limit_bytes=VMEM_LIMIT // 2),
        name="attention",
    )(pos, query, key_all, value_all, pos[:, None])


def attention_back(query, key_all, value_all, d_att, lse, pos, cosine, sine):
    span, cols = query.shape
    head = cosine.shape[1]
    total = key_all.shape[0]
    size = total // 4
    own = pl.BlockSpec((span, head), lambda h, *_: (0, h))
    full = pl.BlockSpec((total, head), lambda h, *_: (0, h))
    same = pl.BlockSpec((span, head), lambda h, *_: (0, 0))
    pos_spec = pl.BlockSpec((span, 1), lambda h, *_: (0, 0))
    flops = 10 * span * total * cols
    return pl.pallas_call(
        attend_back_kernel,
        grid_spec=pltpu.PrefetchScalarGridSpec(
            num_scalar_prefetch=1, grid=(cols // head,),
            in_specs=[own, full, full, own, own, pos_spec, same, same], out_specs=[own, full, full],
            scratch_shapes=[pltpu.VMEM((4, Q_TILE, size), F32)] * 2),
        out_shape=[jax.ShapeDtypeStruct((span, cols), BF16)] + [jax.ShapeDtypeStruct((total, cols), F32)] * 2,
        cost_estimate=pl.CostEstimate(flops=flops, bytes_accessed=16 * total * cols, transcendentals=0),
        compiler_params=pltpu.CompilerParams(vmem_limit_bytes=VMEM_LIMIT // 2),
        name="attention_back",
    )(pos, query, key_all, value_all, d_att, lse, pos[:, None], cosine, sine)


ROW_TILE = 200


def table_kernel(start, order, ids, source, out_ref, grads, sem):
    step = pl.program_id(0)

    @pl.when(step == 0)
    def _():
        copy = pltpu.make_async_copy(source, grads, sem)
        copy.start()
        copy.wait()

    out_ref[...] = jnp.zeros_like(out_ref)
    base = step * out_ref.shape[0]

    def add(i, carry):
        row = pl.ds(ids[i] - base, 1)
        out_ref[row, :] = out_ref[row, :] + grads[pl.ds(order[i], 1), :]
        return carry

    lax.fori_loop(start[step], start[step + 1], add, 0)


def table_grad(ids, order, start, source, rows):
    total, width = source.shape
    tiles = rows // ROW_TILE
    return pl.pallas_call(
        table_kernel,
        grid_spec=pltpu.PrefetchScalarGridSpec(
            num_scalar_prefetch=3, grid=(tiles,), in_specs=[pl.BlockSpec(memory_space=pl.ANY)],
            out_specs=pl.BlockSpec((ROW_TILE, width), lambda i, *_: (i, 0)),
            scratch_shapes=[pltpu.VMEM((total, width), F32), pltpu.SemaphoreType.DMA]),
        out_shape=jax.ShapeDtypeStruct((rows, width), F32),
        cost_estimate=pl.CostEstimate(flops=3 * 10**10, bytes_accessed=4 * rows * width, transcendentals=0),
        compiler_params=pltpu.CompilerParams(vmem_limit_bytes=VMEM_LIMIT // 2),
        name="table_grad",
    )(start, order, ids, source)


def out_proj_kernel(att_ref, w_mine, w_other, embed_ref, res_ref, slots, sems):
    me, x_peer, y_peer, diag = neighbours()
    peers = (x_peer, y_peer)
    enter(peers)
    width = att_ref.shape[1]
    half = att_ref.shape[0] // 2
    sides = [pl.ds(0, half), pl.ds(half, half)]

    cp = lax.axis_index("cp")
    part = w_mine.shape[1]
    tile = 256

    def multiply(block, owner, initial):
        rows = pl.ds(pl.multiple_of(owner * width, width), width)
        for w_ref, base in ((w_mine, cp), (w_other, 1 - cp)):

            def step(j, carry):
                cols = pl.ds(pl.multiple_of(base * part + j * tile, tile), tile)
                term = jnp.dot(block[...], w_ref[rows, pl.ds(pl.multiple_of(j * tile, tile), tile)], preferred_element_type=F32)
                before = embed_ref[:, cols].astype(F32) if initial else res_ref[:, cols]
                res_ref[:, cols] = before + term
                return carry

            lax.fori_loop(0, part // tile, step, 0)

    near = []
    for side in range(2):
        copy = remote(att_ref.at[sides[side]], slots.at[me, sides[side]], sems, side, peers[side])
        copy.start()
        near.append(copy)
    far = []
    for side in range(2):
        copy = remote(att_ref.at[sides[side]], slots.at[me, sides[side]], sems, 2 + side, peers[1 - side])
        copy.start()
        far.append(copy)
    multiply(att_ref, me, True)
    last = []
    for side in range(2):
        near[side].wait_recv()
        owner = peers[side]
        copy = remote(slots.at[owner, sides[side]], slots.at[owner, sides[side]], sems, 4 + side, peers[1 - side])
        copy.start()
        last.append(copy)
    for side in range(2):
        far[side].wait_recv()
    for side in range(2):
        multiply(slots.at[peers[side]], peers[side], False)
    for side in range(2):
        last[side].wait_recv()
    multiply(slots.at[diag], diag, False)
    for copy in near + far + last:
        copy.wait_send()


def out_proj(attended, w_mine, w_other, embed, collective_id):
    span, width = attended.shape
    vmem = pl.BlockSpec(memory_space=pltpu.VMEM)
    return pl.pallas_call(
        out_proj_kernel,
        out_shape=jax.ShapeDtypeStruct(embed.shape, F32),
        in_specs=[vmem] * 4,
        out_specs=vmem,
        scratch_shapes=[pltpu.VMEM((4, span, width), BF16), pltpu.SemaphoreType.DMA((2, 6))],
        compiler_params=pltpu.CompilerParams(
            collective_id=collective_id, has_side_effects=True, vmem_limit_bytes=VMEM_LIMIT),
        cost_estimate=EXCHANGE_COST,
        name="out_proj",
    )(attended, w_mine, w_other, embed)


def solution(mesh):
    cp_count = mesh.shape["cp"]

    def device_step(tokens, pos, doc_id, dy, table, w_q, w_k, w_v, w_o, w_gate, w_up, w_down, gain_one, gain_two, inv_freq):
        span = tokens.shape[0]
        rows = table.shape[0]
        head_dim = 2 * inv_freq.shape[0]
        tp_rank = lax.axis_index("tp")
        gain_a = gain_one.astype(F32)
        gain_b = gain_two.astype(F32)
        swap = [(0, 1), (1, 0)]

        local_ids = tokens - tp_rank * rows
        owned = (local_ids >= 0) & (local_ids < rows)
        safe_ids = jnp.where(owned, local_ids, jnp.arange(span, dtype=jnp.int32) % rows)
        picked = jnp.where(owned[:, None], jnp.take(table, safe_ids, axis=0), jnp.zeros((), BF16))
        half_width = w_o.shape[1] // cp_count
        w_o_half = lax.dynamic_slice_in_dim(w_o, lax.axis_index("cp") * half_width, half_width, axis=1)
        w_o_mine = lax.all_gather(w_o_half, "tp", axis=0, tiled=True)
        w_o_other = lax.ppermute(w_o_mine, "cp", swap)
        all_ids = lax.all_gather(tokens, "cp", axis=0, tiled=True) - tp_rank * rows
        all_ids = jnp.where((all_ids >= 0) & (all_ids < rows), all_ids, rows)
        ids, order = lax.sort((all_ids, jnp.arange(all_ids.shape[0], dtype=jnp.int32)), num_keys=1, is_stable=True)
        edges = jnp.arange(rows // ROW_TILE + 1, dtype=jnp.int32) * ROW_TILE
        starts = jnp.sum((all_ids[None, :] < edges[:, None]).astype(jnp.int32), axis=1)
        angle = pos.astype(F32)[:, None] * inv_freq
        cosine, sine = jnp.cos(angle), jnp.sin(angle)
        cosine = jnp.concatenate([cosine, cosine], axis=1)
        sine = jnp.concatenate([-sine, sine], axis=1)
        embed_b, act_a, query, key_all, value_all = embed_qkv(picked, gain_a[None, :], w_q, w_k, w_v, cosine, sine, cp_count, 0)
        attended, lse = attention(query, key_all, value_all, pos, head_dim)
        residual = out_proj(attended, w_o_mine, w_o_other, embed_b, 1)
        normed_b, inv_b = rms_stats(residual)
        act_b = (normed_b * gain_b).astype(BF16)
        gate = jnp.dot(act_b, w_gate, preferred_element_type=F32)
        up_val = jnp.dot(act_b, w_up, preferred_element_type=F32)
        gate_sig = jax.nn.sigmoid(gate)
        hidden = (gate * gate_sig * up_val).astype(BF16)
        d_hidden = to_bf16(jnp.einsum("td,fd->tf", dy, w_down, preferred_element_type=F32))
        d_gate = (d_hidden * up_val * gate_sig * (1.0 + gate * (1.0 - gate_sig))).astype(BF16)
        d_up = (d_hidden * gate * gate_sig).astype(BF16)
        d_act_b = grad_b(d_gate, d_up, w_gate.T, w_up.T, 2)

        hidden, d_act_b = lax.optimization_barrier((hidden, d_act_b))
        out_part = jnp.dot(hidden, w_down, preferred_element_type=F32)
        out_mine = lax.psum_scatter(out_part, "tp", scatter_dimension=0, tiled=True)

        grad_down = jnp.einsum("tf,td->fd", hidden, dy, preferred_element_type=F32)
        grad_gate = jnp.einsum("tf,td->fd", d_gate, act_b, preferred_element_type=F32)
        grad_up = jnp.einsum("tf,td->fd", d_up, act_b, preferred_element_type=F32)
        d_act_b = d_act_b.astype(F32)
        grad_gain_b = jnp.sum(d_act_b * normed_b, axis=0)
        d_resid = dy.astype(F32) + rms_back(d_act_b * gain_b, normed_b, inv_b)
        d_resid_b = d_resid.astype(BF16)
        grad_out = jnp.einsum("tc,td->cd", attended, d_resid_b, preferred_element_type=F32)
        d_att = jnp.einsum("td,cd->tc", d_resid_b, w_o, preferred_element_type=F32).astype(BF16)
        d_q_pre, d_key_all, d_value_all = attention_back(query, key_all, value_all, d_att, lse, pos, cosine, sine)
        out_mine, d_q_pre, grad_gate, grad_up, grad_down = lax.optimization_barrier(
            (out_mine, d_q_pre, grad_gate, grad_up, grad_down))
        grad_gate, grad_up, grad_down = lax.psum((grad_gate, grad_up, grad_down), "cp")
        d_embed, grad_gain_a, d_k_pre, d_v_pre = grad_a(
            d_q_pre, d_key_all, d_value_all, w_q, w_k, w_v, cosine, sine, embed_b, gain_a[None, :], d_resid, cp_count, 3)
        grad_gain_a = grad_gain_a[0]
        out_mine, d_embed = lax.optimization_barrier((out_mine, d_embed))
        res_mine = lax.dynamic_slice_in_dim(residual, tp_rank * (span // 4), span // 4, axis=0)
        layer_out = lax.all_gather((out_mine + res_mine).astype(BF16), "tp", axis=0, tiled=True)
        grad_table = table_grad(ids, order, starts, d_embed, rows)
        grad_q = jnp.einsum("td,tc->dc", act_a, d_q_pre, preferred_element_type=F32)
        grad_k = jnp.einsum("td,tc->dc", act_a, d_k_pre, preferred_element_type=F32)
        grad_v = jnp.einsum("td,tc->dc", act_a, d_v_pre, preferred_element_type=F32)
        (grad_q, grad_k, grad_v, grad_out), (grad_gate, grad_up, grad_down) = lax.optimization_barrier(
            ((grad_q, grad_k, grad_v, grad_out), (grad_gate, grad_up, grad_down)))
        att_grads = lax.psum((grad_q, grad_k, grad_v, grad_out), "cp")
        gains = lax.psum((grad_gain_a, grad_gain_b), "cp")
        return (layer_out, grad_table) + tuple(att_grads) + (grad_gate.T, grad_up.T, grad_down) + tuple(gains)

    col_spec = P(None, "tp")
    row_spec = P("tp", None)
    tok_spec = P("cp")
    rep_spec = P(None)
    in_specs = (tok_spec, tok_spec, tok_spec, P("cp", None), row_spec, col_spec, col_spec, col_spec, row_spec, col_spec, col_spec, row_spec, rep_spec, rep_spec, rep_spec)
    out_specs = (P("cp", None), row_spec, col_spec, col_spec, col_spec, row_spec, col_spec, col_spec, row_spec, rep_spec, rep_spec)
    return jax.shard_map(device_step, mesh=mesh, in_specs=in_specs, out_specs=out_specs, check_vma=False)
```

```python
import functools

import jax
import jax.numpy as jnp
from jax import lax
from jax.experimental import pallas as pl
from jax.experimental.pallas import tpu as pltpu
from jax.sharding import PartitionSpec as P


NORM_EPS = 1e-5
NEG_BIG = -1e30
MESH = pl.DeviceIdType.MESH
NN = (((1,), (0,)), ((), ()))
NT = (((1,), (1,)), ((), ()))
VMEM_LIMIT = 60 * 1024 * 1024
F32 = jnp.float32
BF16 = jnp.bfloat16


def rms_stats(feats):
    inv_rms = lax.rsqrt(jnp.mean(feats * feats, axis=-1, keepdims=True) + NORM_EPS)
    return feats * inv_rms, inv_rms


def rms_back(d_normed, normed, inv_rms):
    return inv_rms * (d_normed - normed * jnp.mean(d_normed * normed, axis=-1, keepdims=True))


def to_bf16(feats):
    return feats.astype(BF16).astype(F32)


def neighbours():
    me = lax.axis_index("tp")
    return me, me + 1 - 2 * lax.rem(me, 2), lax.rem(me + 2, 4), 3 - me


def enter(peers):
    barrier = pltpu.get_barrier_semaphore()
    for peer in peers:
        pl.semaphore_signal(barrier, inc=1, device_id={"tp": peer}, device_id_type=MESH)
    pl.semaphore_wait(barrier, len(peers))


def remote(src, dst, sems, slot, peer):
    return pltpu.make_async_remote_copy(
        src_ref=src, dst_ref=dst, send_sem=sems.at[0, slot], recv_sem=sems.at[1, slot],
        device_id={"tp": peer}, device_id_type=MESH)


def tp_exchange(compute, done, out_ref, part, recv1, recv2, sems):
    wide = part.dtype
    block, half = part.shape[2], part.shape[3]
    me, x_peer, y_peer, diag = neighbours()
    peers = (x_peer, y_peer)

    first = []
    for k in range(2):
        for side in range(2):
            owner = diag if k == 0 else peers[side]
            compute(side, owner)
            copy = remote(part.at[side, owner], recv1.at[side, k], sems, side * 2 + k, peers[side])
            copy.start()
            first.append(copy)
    for side in range(2):
        compute(side, peers[1 - side])
    for side in range(2):
        compute(side, me)
    second = []
    for side in range(2):
        first[side].wait_recv()
        owner = peers[1 - side]
        part[side, owner] = (part[side, owner].astype(F32) + recv1[side, 0].astype(F32)).astype(wide)
        copy = remote(part.at[side, owner], recv2.at[side], sems, 4 + side, peers[1 - side])
        copy.start()
        second.append(copy)
    mine = pl.ds(pl.multiple_of(me * block, block), block)
    sides = [slice(side * half, (side + 1) * half) for side in range(2)]
    own = []
    for side in range(2):
        first[2 + side].wait_recv()
        second[side].wait_recv()
        total = part[side, me].astype(F32) + recv1[side, 1].astype(F32) + recv2[side].astype(F32)
        out_ref[mine, sides[side]] = total.astype(out_ref.dtype)
        copy = remote(out_ref.at[mine, sides[side]], out_ref.at[mine, sides[side]], sems, 6 + side, peers[1 - side])
        copy.start()
        own.append(copy)
    far = []
    for side in range(2):
        copy = remote(out_ref.at[mine, sides[side]], out_ref.at[mine, sides[side]], sems, 8 + side, peers[side])
        copy.start()
        far.append(copy)
    done(me)
    for side in range(2):
        own[side].wait_recv()
        rows = pl.ds(pl.multiple_of(peers[1 - side] * block, block), block)
        copy = remote(out_ref.at[rows, sides[side]], out_ref.at[rows, sides[side]], sems, 10 + side, peers[side])
        copy.start()
        far.append(copy)
    for side in range(2):
        far[side].wait_recv()
    done(x_peer)
    done(y_peer)
    for side in range(2):
        far[2 + side].wait_recv()
    done(diag)
    for copy in first + second + own + far:
        copy.wait_send()


def exchange_scratch(span, width, wide):
    block, half = span // 4, width // 2
    return [
        pltpu.VMEM((2, 4, block, half), wide),
        pltpu.VMEM((2, 2, block, half), wide),
        pltpu.VMEM((2, block, half), wide),
        pltpu.SemaphoreType.DMA((2, 12)),
    ]


EXCHANGE_COST = pl.CostEstimate(flops=10**11, bytes_accessed=10**8, transcendentals=0)


def comm_params(collective_id, mib=60):
    return pltpu.CompilerParams(collective_id=collective_id, has_side_effects=True, vmem_limit_bytes=mib * 1024 * 1024)


VMEM_SPEC = pl.BlockSpec(memory_space=pltpu.VMEM)


def product_into(part, lhs, rhs, dims, bases):
    block, half = part.shape[2], part.shape[3]
    tile = 256

    def compute(side, owner):

        def step(j, carry):
            total = None
            for left, right, base in zip(lhs, rhs, bases):
                rows = pl.ds(pl.multiple_of(base + owner * block, block), block)
                start = pl.multiple_of(side * half + j * tile, tile)
                piece = right[pl.ds(start, tile), :] if dims == NT else right[:, pl.ds(start, tile)]
                term = lax.dot_general(left[rows, :], piece, dims, preferred_element_type=F32)
                total = term if total is None else total + term
            part[side, owner, :, pl.ds(pl.multiple_of(j * tile, tile), tile)] = total
            return carry

        lax.fori_loop(0, half // tile, step, 0)

    return compute


def inverse_root(value):
    guess = lax.rsqrt(value)
    return guess * (1.5 - 0.5 * value * guess * guess)


def turn(feats, cosine, sine):
    return feats * cosine + pltpu.roll(feats, feats.shape[-1] // 2, 1) * sine


def embed_kernel(picked, owned, gain, w_q, w_k, w_v, cosine, sine, embed, act, act_all, q_ref, k_ref, v_ref, part, recv1, recv2, sems, kv_sems):
    block, half = part.shape[2], part.shape[3]
    span = picked.shape[0]
    head = cosine.shape[1]
    me, x_peer, y_peer, diag = neighbours()
    cp = lax.axis_index("cp")
    barrier = pltpu.get_barrier_semaphore()
    for peer in ({"tp": x_peer}, {"tp": y_peer}, {"cp": 1 - cp}):
        pl.semaphore_signal(barrier, inc=1, device_id=peer, device_id_type=MESH)
    pl.semaphore_wait(barrier, 3)
    sent = []

    def compute(side, owner):
        rows = pl.ds(pl.multiple_of(owner * block, block), block)
        part[side, owner] = (picked[rows, side * half:(side + 1) * half].astype(F32) * owned[rows, :]).astype(BF16)

    def done(owner):
        rows = pl.ds(pl.multiple_of(owner * block, block), block)
        slots = pl.ds(pl.multiple_of(cp * span + owner * block, block), block)
        feats = embed[rows, :].astype(F32)
        inv_rms = inverse_root(jnp.mean(feats * feats, axis=-1, keepdims=True) + NORM_EPS)
        normed = (feats * inv_rms * gain[...]).astype(BF16)
        act[rows, :] = normed
        act_all[slots, :] = normed

        def step(j, carry):
            cols = pl.ds(pl.multiple_of(j * head, head), head)
            left = act[rows, :]
            query = jnp.dot(left, w_q[:, cols], preferred_element_type=F32)
            q_ref[rows, cols] = turn(query, cosine[rows, :], sine[rows, :]).astype(BF16)
            key = jnp.dot(left, w_k[:, cols], preferred_element_type=F32)
            k_ref[slots, cols] = turn(key, cosine[rows, :], sine[rows, :]).astype(BF16)
            v_ref[slots, cols] = jnp.dot(left, w_v[:, cols], preferred_element_type=F32).astype(BF16)
            return carry

        lax.fori_loop(0, w_q.shape[1] // head, step, 0)
        for ref in (k_ref, v_ref, act_all):
            slot = len(sent)
            copy = pltpu.make_async_remote_copy(
                src_ref=ref.at[slots], dst_ref=ref.at[slots], send_sem=kv_sems.at[0, slot], recv_sem=kv_sems.at[1, slot],
                device_id={"cp": 1 - cp}, device_id_type=MESH)
            copy.start()
            sent.append(copy)

    tp_exchange(compute, done, embed, part, recv1, recv2, sems)
    for copy in sent:
        copy.wait_recv()
    for copy in sent:
        copy.wait_send()


def embed_qkv(picked, owned, gain, w_q, w_k, w_v, cosine, sine, cp_count, collective_id):
    span, width = picked.shape
    cols = w_q.shape[1]
    return pl.pallas_call(
        embed_kernel,
        out_shape=[jax.ShapeDtypeStruct(shape, BF16) for shape in (
            (span, width), (span, width), (span * cp_count, width), (span, cols), (span * cp_count, cols), (span * cp_count, cols))],
        in_specs=[VMEM_SPEC] * 8,
        out_specs=[VMEM_SPEC] * 6,
        scratch_shapes=exchange_scratch(span, width, BF16) + [pltpu.SemaphoreType.DMA((2, 12))],
        compiler_params=comm_params(collective_id, 48),
        cost_estimate=EXCHANGE_COST,
        name="embed_qkv",
    )(picked, owned, gain, w_q, w_k, w_v, cosine, sine)


def grad_b_kernel(d_gate, d_up, w_gate, w_up, out, part, recv1, recv2, sems):
    enter(neighbours()[1:3])
    tp_exchange(product_into(part, (d_gate, d_up), (w_gate, w_up), NN, (0, 0)), lambda owner: None, out, part, recv1, recv2, sems)


def grad_b(d_gate, d_up, w_gate_t, w_up_t, collective_id):
    span, width = d_gate.shape[0], w_gate_t.shape[1]
    return pl.pallas_call(
        grad_b_kernel,
        out_shape=jax.ShapeDtypeStruct((span, width), BF16),
        in_specs=[VMEM_SPEC] * 4,
        out_specs=VMEM_SPEC,
        scratch_shapes=exchange_scratch(span, width, F32),
        compiler_params=comm_params(collective_id, 42),
        cost_estimate=EXCHANGE_COST,
        name="grad_b",
    )(d_gate, d_up, w_gate_t, w_up_t)


def grad_a_kernel(
    d_q, d_k_all, d_v_all, w_q, w_k, w_v, cosine, sine, embed, gain, gain_b_part, d_resid,
    d_embed, grad_gain, grad_gain_b, d_k, d_v, out, resid, recv_k, recv_v, part, recv1, recv2, sems, kv_sems, row_sems, gain_part, gain_other, own_k, own_v):
    span = d_q.shape[0]
    block = part.shape[2]
    head = cosine.shape[1]
    me, x_peer, y_peer, diag = neighbours()
    cp = lax.axis_index("cp")
    barrier = pltpu.get_barrier_semaphore()
    for peer in ({"tp": x_peer}, {"tp": y_peer}, {"cp": 1 - cp}):
        pl.semaphore_signal(barrier, inc=1, device_id=peer, device_id_type=MESH)
    pl.semaphore_wait(barrier, 3)
    load = pltpu.make_async_copy(d_resid, resid, row_sems.at[0, 0])
    load.start()
    held = pl.ds(pl.multiple_of(cp * span, span), span)
    loads = [
        pltpu.make_async_copy(source.at[held], target, row_sems.at[3, 2 + which])
        for which, (source, target) in enumerate(((d_k_all, own_k), (d_v_all, own_v)))]
    for copy in loads:
        copy.start()
    trades = []
    for which, source in enumerate((gain_b_part, gain_part)):
        trades.append(pltpu.make_async_remote_copy(
            src_ref=source, dst_ref=gain_other.at[which], send_sem=row_sems.at[3, which], recv_sem=row_sems.at[4, which],
            device_id={"cp": 1 - cp}, device_id_type=MESH))
    trades[0].start()
    order = (diag, x_peer, y_peer, me)
    copies = []
    for place, owner in enumerate(order):
        rows = pl.ds(pl.multiple_of(owner * block, block), block)
        theirs = pl.ds(pl.multiple_of((1 - cp) * span + owner * block, block), block)
        for which, (source, target) in enumerate(((d_k_all, recv_k), (d_v_all, recv_v))):
            slot = 2 * place + which
            copy = pltpu.make_async_remote_copy(
                src_ref=source.at[theirs], dst_ref=target.at[rows], send_sem=kv_sems.at[0, slot], recv_sem=kv_sems.at[1, slot],
                device_id={"cp": 1 - cp}, device_id_type=MESH)
            copy.start()
            copies.append(copy)
    product = product_into(part, (d_q, d_k, d_v), (w_q, w_k, w_v), NT, (0, cp * span, cp * span))
    ready = []

    def prepare(place):
        owner = order[place]
        if place == 0:
            for copy in loads:
                copy.wait()
        copies[2 * place].wait_recv()
        copies[2 * place + 1].wait_recv()
        rows = pl.ds(pl.multiple_of(owner * block, block), block)
        ours = pl.ds(pl.multiple_of(cp * span + owner * block, block), block)

        def step(j, carry):
            cols = pl.ds(pl.multiple_of(j * head, head), head)
            total = (own_k[rows, cols] + recv_k[rows, cols]).astype(BF16).astype(F32)
            d_k[ours, cols] = turn(total, cosine[rows, :], -sine[rows, :]).astype(BF16)
            d_v[ours, cols] = (own_v[rows, cols] + recv_v[rows, cols]).astype(BF16)
            return carry

        lax.fori_loop(0, d_q.shape[1] // head, step, 0)
        for which, ref in enumerate((d_k, d_v)):
            slot = 8 + 2 * place + which
            copy = pltpu.make_async_remote_copy(
                src_ref=ref.at[ours], dst_ref=ref.at[ours], send_sem=kv_sems.at[0, slot], recv_sem=kv_sems.at[1, slot],
                device_id={"cp": 1 - cp}, device_id_type=MESH)
            copy.start()
            ready.append(copy)

    calls = []

    def compute(side, owner):
        turn_no = len(calls)
        calls.append(side)
        if turn_no == 0:
            prepare(0)
        elif turn_no == 2:
            prepare(1)
        elif turn_no == 3:
            prepare(2)
        elif turn_no == 6:
            prepare(3)
        product(side, owner)

    gain_part[...] = jnp.zeros_like(gain_part)
    local, shared = [], []

    def done(owner):
        if not local:
            load.wait()
        rows = pl.ds(pl.multiple_of(owner * block, block), block)
        slots = pl.ds(pl.multiple_of(cp * span + owner * block, block), block)
        feats = embed[rows, :].astype(F32)
        inv_rms = inverse_root(jnp.mean(feats * feats, axis=-1, keepdims=True) + NORM_EPS)
        normed = feats * inv_rms
        d_act = out[rows, :].astype(F32)
        gain_part[...] = gain_part[...] + jnp.sum(d_act * normed, axis=0, keepdims=True)
        resid[rows, :] = resid[rows, :] + rms_back(d_act * gain[...], normed, inv_rms)
        slot = 1 + len(local)
        copy = pltpu.make_async_copy(resid.at[rows], d_embed.at[slots], row_sems.at[0, slot])
        copy.start()
        local.append(copy)
        copy = pltpu.make_async_remote_copy(
            src_ref=resid.at[rows], dst_ref=d_embed.at[slots], send_sem=row_sems.at[1, slot], recv_sem=row_sems.at[2, slot],
            device_id={"cp": 1 - cp}, device_id_type=MESH)
        copy.start()
        shared.append(copy)

    tp_exchange(compute, done, out, part, recv1, recv2, sems)
    trades[1].start()
    for copy in local:
        copy.wait()
    for copy in trades:
        copy.wait_recv()
    grad_gain[...] = gain_part[...] + gain_other[1]
    grad_gain_b[...] = gain_b_part[...] + gain_other[0]
    for copy in shared + ready:
        copy.wait_recv()
    for copy in copies + shared + ready + trades:
        copy.wait_send()


def grad_a(d_q, d_k_all, d_v_all, w_q, w_k, w_v, cosine, sine, embed, gain, gain_b_part, d_resid, cp_count, collective_id):
    span, width = d_q.shape[0], w_q.shape[0]
    cols = d_q.shape[1]
    hbm = pl.BlockSpec(memory_space=pl.ANY)
    return pl.pallas_call(
        grad_a_kernel,
        out_shape=[
            jax.ShapeDtypeStruct((span * cp_count, width), F32), jax.ShapeDtypeStruct((1, width), F32),
            jax.ShapeDtypeStruct((1, width), F32)] + [jax.ShapeDtypeStruct((span * cp_count, cols), BF16)] * 2,
        in_specs=[VMEM_SPEC] + [hbm] * 2 + [VMEM_SPEC] * 8 + [hbm],
        out_specs=[hbm] + [VMEM_SPEC] * 4,
        scratch_shapes=[pltpu.VMEM((span, width), BF16), pltpu.VMEM((span, width), F32)] + [pltpu.VMEM((span, cols), F32)] * 2
        + exchange_scratch(span, width, F32) + [pltpu.SemaphoreType.DMA((2, 16)), pltpu.SemaphoreType.DMA((5, 5))]
        + [pltpu.VMEM((1, width), F32), pltpu.VMEM((2, 1, width), F32)]
        + [pltpu.VMEM((span, cols), F32)] * 2,
        compiler_params=comm_params(collective_id),
        cost_estimate=EXCHANGE_COST,
        name="grad_a",
    )(d_q, d_k_all, d_v_all, w_q, w_k, w_v, cosine, sine, embed, gain, gain_b_part, d_resid)


Q_TILE = 256


def key_row(chunk, size):
    return pl.multiple_of(jnp.where(chunk < 2, 2 * chunk, 7 - 2 * chunk) * size, size)


def query_plan(i, size, pos_smem):
    cp = lax.axis_index("cp")
    per_block = size // Q_TILE
    seq_block = jnp.where(i < per_block, cp, 3 - cp)
    start = seq_block * size + lax.rem(i, per_block) * Q_TILE
    low = jnp.maximum(start - pos_smem[i * Q_TILE], 0) // size
    return start, low, seq_block + 1


def distance(size):
    return lax.broadcasted_iota(jnp.int32, (Q_TILE, size), 0) - lax.broadcasted_iota(jnp.int32, (Q_TILE, size), 1)


def attend_kernel(pos_smem, q_ref, k_ref, v_ref, pos_ref, o_ref, lse_ref, held):
    size = held.shape[2]
    head = q_ref.shape[1]
    scale = head ** -0.5

    def block(i, carry):
        start, low, high = query_plan(i, size, pos_smem)
        rows = pl.ds(pl.multiple_of(i * Q_TILE, Q_TILE), Q_TILE)
        query = q_ref[rows, :]
        back = pos_ref[rows, :]

        def score(c, top):
            keys = k_ref[pl.ds(key_row(c, size), size), :]
            scores = lax.dot_general(query, keys, NT, preferred_element_type=F32) * scale
            gap = distance(size) + (start - c * size)
            scores = jnp.where((gap >= 0) & (gap <= back), scores, NEG_BIG)
            held[c] = scores
            return jnp.maximum(top, jnp.max(scores, axis=1, keepdims=True))

        top = lax.fori_loop(low, high, score, jnp.full((Q_TILE, 1), NEG_BIG, F32))

        def expo(c, total):
            prob = jnp.exp(held[c] - top)
            held[c] = prob
            return total + jnp.sum(prob, axis=1, keepdims=True)

        total = lax.fori_loop(low, high, expo, jnp.zeros((Q_TILE, 1), F32))
        share = 1.0 / total

        def gather(c, acc):
            prob = (held[c] * share).astype(BF16)
            values = v_ref[pl.ds(key_row(c, size), size), :]
            return acc + jnp.dot(prob, values, preferred_element_type=F32)

        acc = lax.fori_loop(low, high, gather, jnp.zeros((Q_TILE, head), F32))
        o_ref[rows, :] = acc.astype(BF16)
        lse_ref[rows, :] = jnp.broadcast_to(top + jnp.log(total), (Q_TILE, head))
        return carry

    lax.fori_loop(0, q_ref.shape[0] // Q_TILE, block, 0)


def attend_back_kernel(pos_smem, q_ref, k_ref, v_ref, do_ref, lse_ref, pos_ref, cosine, sine, dq_ref, dk_ref, dv_ref, held_p, held_d):
    size = held_p.shape[2]
    head = q_ref.shape[1]
    scale = head ** -0.5
    dk_ref[...] = jnp.zeros_like(dk_ref)
    dv_ref[...] = jnp.zeros_like(dv_ref)
    over_rows = (((0,), (0,)), ((), ()))

    def block(i, carry):
        start, low, high = query_plan(i, size, pos_smem)
        rows = pl.ds(pl.multiple_of(i * Q_TILE, Q_TILE), Q_TILE)
        query = q_ref[rows, :]
        d_out = do_ref[rows, :]
        lse = lse_ref[rows, :][:, :1]
        back = pos_ref[rows, :]

        def probs(c, total):
            place = pl.ds(key_row(c, size), size)
            scores = lax.dot_general(query, k_ref[place, :], NT, preferred_element_type=F32) * scale
            gap = distance(size) + (start - c * size)
            prob = jnp.where((gap >= 0) & (gap <= back), jnp.exp(scores - lse), 0.0)
            d_prob = to_bf16(lax.dot_general(d_out, v_ref[place, :], NT, preferred_element_type=F32))
            held_p[c] = prob
            held_d[c] = d_prob
            return total + jnp.sum(prob * d_prob, axis=1, keepdims=True)

        mean = lax.fori_loop(low, high, probs, jnp.zeros((Q_TILE, 1), F32))

        def grads(c, acc):
            place = pl.ds(key_row(c, size), size)
            prob = held_p[c]
            d_score = (prob * (held_d[c] - mean) * scale).astype(BF16)
            dk_ref[place, :] = dk_ref[place, :] + lax.dot_general(d_score, query, over_rows, preferred_element_type=F32)
            dv_ref[place, :] = dv_ref[place, :] + lax.dot_general(prob.astype(BF16), d_out, over_rows, preferred_element_type=F32)
            return acc + jnp.dot(d_score, k_ref[place, :], preferred_element_type=F32)

        d_query = lax.fori_loop(low, high, grads, jnp.zeros((Q_TILE, head), F32))
        dq_ref[rows, :] = turn(to_bf16(d_query), cosine[rows, :], -sine[rows, :]).astype(BF16)
        return carry

    lax.fori_loop(0, q_ref.shape[0] // Q_TILE, block, 0)


def attention(query, key_all, value_all, pos, head):
    span, cols = query.shape
    total = key_all.shape[0]
    size = total // 4
    own = pl.BlockSpec((span, head), lambda h, *_: (0, h))
    full = pl.BlockSpec((total, head), lambda h, *_: (0, h))
    pos_spec = pl.BlockSpec((span, 1), lambda h, *_: (0, 0))
    flops = 4 * span * total * cols
    return pl.pallas_call(
        attend_kernel,
        grid_spec=pltpu.PrefetchScalarGridSpec(
            num_scalar_prefetch=1, grid=(cols // head,), in_specs=[own, full, full, pos_spec], out_specs=[own, own],
            scratch_shapes=[pltpu.VMEM((4, Q_TILE, size), F32)]),
        out_shape=[jax.ShapeDtypeStruct((span, cols), BF16), jax.ShapeDtypeStruct((span, cols), F32)],
        cost_estimate=pl.CostEstimate(flops=flops, bytes_accessed=8 * total * cols, transcendentals=0),
        compiler_params=pltpu.CompilerParams(vmem_limit_bytes=VMEM_LIMIT // 2),
        name="attention",
    )(pos, query, key_all, value_all, pos[:, None])


def attention_back(query, key_all, value_all, d_att, lse, pos, cosine, sine):
    span, cols = query.shape
    head = cosine.shape[1]
    total = key_all.shape[0]
    size = total // 4
    own = pl.BlockSpec((span, head), lambda h, *_: (0, h))
    full = pl.BlockSpec((total, head), lambda h, *_: (0, h))
    same = pl.BlockSpec((span, head), lambda h, *_: (0, 0))
    pos_spec = pl.BlockSpec((span, 1), lambda h, *_: (0, 0))
    flops = 10 * span * total * cols
    return pl.pallas_call(
        attend_back_kernel,
        grid_spec=pltpu.PrefetchScalarGridSpec(
            num_scalar_prefetch=1, grid=(cols // head,),
            in_specs=[own, full, full, own, own, pos_spec, same, same], out_specs=[own, full, full],
            scratch_shapes=[pltpu.VMEM((4, Q_TILE, size), F32)] * 2),
        out_shape=[jax.ShapeDtypeStruct((span, cols), BF16)] + [jax.ShapeDtypeStruct((total, cols), F32)] * 2,
        cost_estimate=pl.CostEstimate(flops=flops, bytes_accessed=16 * total * cols, transcendentals=0),
        compiler_params=pltpu.CompilerParams(vmem_limit_bytes=VMEM_LIMIT // 2),
        name="attention_back",
    )(pos, query, key_all, value_all, d_att, lse, pos[:, None], cosine, sine)


ROW_TILE = 200


PASS_TILES = 16


def table_kernel(count, start, order, ids, source, *refs):
    passed, out_ref, written, grads, sem = refs[:count], refs[count], refs[count + 1:2 * count + 1], refs[-2], refs[-1]
    step = pl.program_id(0)

    @pl.when(step == 0)
    def _():
        copy = pltpu.make_async_copy(source, grads, sem)
        copy.start()
        copy.wait()

    @pl.when(step < PASS_TILES)
    def _():
        for left, right in zip(passed, written):
            right[...] = left[...]

    out_ref[...] = jnp.zeros_like(out_ref)
    base = step * out_ref.shape[0]

    def add(i, carry):
        row = pl.ds(ids[i] - base, 1)
        out_ref[row, :] = out_ref[row, :] + grads[pl.ds(order[i], 1), :]
        return carry

    lax.fori_loop(start[step], start[step + 1], add, 0)


def table_grad(ids, order, start, source, rows, passed):
    total, width = source.shape
    tiles = rows // ROW_TILE
    specs = []
    for array in passed:
        if array.shape[1] == width:
            specs.append(pl.BlockSpec((array.shape[0], width // PASS_TILES), lambda i, *_: (0, jnp.minimum(i, PASS_TILES - 1))))
        else:
            specs.append(pl.BlockSpec((array.shape[0] // PASS_TILES, array.shape[1]), lambda i, *_: (jnp.minimum(i, PASS_TILES - 1), 0)))
    return pl.pallas_call(
        functools.partial(table_kernel, len(passed)),
        grid_spec=pltpu.PrefetchScalarGridSpec(
            num_scalar_prefetch=3, grid=(tiles,), in_specs=[pl.BlockSpec(memory_space=pl.ANY)] + specs,
            out_specs=[pl.BlockSpec((ROW_TILE, width), lambda i, *_: (i, 0))] + specs,
            scratch_shapes=[pltpu.VMEM((total, width), F32), pltpu.SemaphoreType.DMA]),
        out_shape=[jax.ShapeDtypeStruct((rows, width), F32)] + [jax.ShapeDtypeStruct(array.shape, F32) for array in passed],
        cost_estimate=pl.CostEstimate(flops=4 * 10**10, bytes_accessed=4 * rows * width, transcendentals=0),
        compiler_params=pltpu.CompilerParams(vmem_limit_bytes=VMEM_LIMIT * 3 // 4),
        name="table_grad",
    )(start, order, ids, source, *passed)


def out_proj_kernel(att_ref, w_mine, w_other, embed_ref, dy_ref, w_down, res_ref, d_hidden, slots, sems):
    me, x_peer, y_peer, diag = neighbours()
    peers = (x_peer, y_peer)
    enter(peers)
    width = att_ref.shape[1]
    half = att_ref.shape[0] // 2
    sides = [pl.ds(0, half), pl.ds(half, half)]

    cp = lax.axis_index("cp")
    part = w_mine.shape[1]
    tile = 256

    def multiply(block, owner, initial):
        rows = pl.ds(pl.multiple_of(owner * width, width), width)
        for w_ref, base in ((w_mine, cp), (w_other, 1 - cp)):

            def step(j, carry):
                cols = pl.ds(pl.multiple_of(base * part + j * tile, tile), tile)
                term = jnp.dot(block[...], w_ref[rows, pl.ds(pl.multiple_of(j * tile, tile), tile)], preferred_element_type=F32)
                before = embed_ref[:, cols].astype(F32) if initial else res_ref[:, cols]
                res_ref[:, cols] = before + term
                return carry

            lax.fori_loop(0, part // tile, step, 0)

    near = []
    for side in range(2):
        copy = remote(att_ref.at[sides[side]], slots.at[me, sides[side]], sems, side, peers[side])
        copy.start()
        near.append(copy)
    far = []
    for side in range(2):
        copy = remote(att_ref.at[sides[side]], slots.at[me, sides[side]], sems, 2 + side, peers[1 - side])
        copy.start()
        far.append(copy)
    multiply(att_ref, me, True)
    last = []
    for side in range(2):
        near[side].wait_recv()
        owner = peers[side]
        copy = remote(slots.at[owner, sides[side]], slots.at[owner, sides[side]], sems, 4 + side, peers[1 - side])
        copy.start()
        last.append(copy)

    def back(i, carry):
        rows = pl.ds(pl.multiple_of(i * 128, 128), 128)
        d_hidden[rows, :] = lax.dot_general(dy_ref[rows, :], w_down[...], NT, preferred_element_type=F32).astype(BF16)
        return carry

    lax.fori_loop(0, dy_ref.shape[0] // 128, back, 0)
    for side in range(2):
        far[side].wait_recv()
    for side in range(2):
        multiply(slots.at[peers[side]], peers[side], False)
    for side in range(2):
        last[side].wait_recv()
    multiply(slots.at[diag], diag, False)
    for copy in near + far + last:
        copy.wait_send()


def out_proj(attended, w_mine, w_other, embed, dy, w_down, collective_id):
    span, width = attended.shape
    return pl.pallas_call(
        out_proj_kernel,
        out_shape=[jax.ShapeDtypeStruct(embed.shape, F32), jax.ShapeDtypeStruct((span, w_down.shape[0]), BF16)],
        in_specs=[VMEM_SPEC] * 6,
        out_specs=[VMEM_SPEC] * 2,
        scratch_shapes=[pltpu.VMEM((4, span, width), BF16), pltpu.SemaphoreType.DMA((2, 6))],
        compiler_params=comm_params(collective_id, 46),
        cost_estimate=EXCHANGE_COST,
        name="out_proj",
    )(attended, w_mine, w_other, embed, dy, w_down)


def solution(mesh):
    cp_count = mesh.shape["cp"]

    def device_step(tokens, pos, doc_id, dy, table, w_q, w_k, w_v, w_o, w_gate, w_up, w_down, gain_one, gain_two, inv_freq):
        span = tokens.shape[0]
        rows = table.shape[0]
        head_dim = 2 * inv_freq.shape[0]
        tp_rank = lax.axis_index("tp")
        gain_a = gain_one.astype(F32)
        gain_b = gain_two.astype(F32)
        swap = [(0, 1), (1, 0)]

        local_ids = tokens - tp_rank * rows
        owned = (local_ids >= 0) & (local_ids < rows)
        safe_ids = jnp.where(owned, local_ids, jnp.arange(span, dtype=jnp.int32) % rows)
        picked = jnp.take(table, safe_ids, axis=0, mode="clip")
        half_width = w_o.shape[1] // cp_count
        w_o_half = lax.dynamic_slice_in_dim(w_o, lax.axis_index("cp") * half_width, half_width, axis=1)
        w_o_mine = lax.all_gather(w_o_half, "tp", axis=0, tiled=True)
        all_ids = lax.all_gather(tokens, "cp", axis=0, tiled=True) - tp_rank * rows
        all_ids = jnp.where((all_ids >= 0) & (all_ids < rows), all_ids, rows)
        ids, order = lax.sort((all_ids, jnp.arange(all_ids.shape[0], dtype=jnp.int32)), num_keys=1, is_stable=True)
        edges = jnp.arange(rows // ROW_TILE + 1, dtype=jnp.int32) * ROW_TILE
        starts = jnp.sum((all_ids[None, :] < edges[:, None]).astype(jnp.int32), axis=1)
        angle = pos.astype(F32)[:, None] * inv_freq
        cosine, sine = jnp.cos(angle), jnp.sin(angle)
        cosine = jnp.concatenate([cosine, cosine], axis=1)
        sine = jnp.concatenate([-sine, sine], axis=1)
        embed_b, act_a, act_all, query, key_all, value_all = embed_qkv(
            picked, owned.astype(F32)[:, None], gain_a[None, :], w_q, w_k, w_v, cosine, sine, cp_count, 0)
        w_o_mine, query = lax.optimization_barrier((w_o_mine, query))
        w_o_other = lax.ppermute(w_o_mine, "cp", swap)
        attended, lse = attention(query, key_all, value_all, pos, head_dim)
        residual, d_hidden = out_proj(attended, w_o_mine, w_o_other, embed_b, dy, w_down, 1)
        normed_b, inv_b = rms_stats(residual)
        act_b = (normed_b * gain_b).astype(BF16)
        gate = jnp.dot(act_b, w_gate, preferred_element_type=F32)
        up_val = jnp.dot(act_b, w_up, preferred_element_type=F32)
        gate_sig = jax.nn.sigmoid(gate)
        hidden = (gate * gate_sig * up_val).astype(BF16)
        d_hidden = d_hidden.astype(F32)
        d_gate = (d_hidden * up_val * gate_sig * (1.0 + gate * (1.0 - gate_sig))).astype(BF16)
        d_up = (d_hidden * gate * gate_sig).astype(BF16)
        d_act_b = grad_b(d_gate, d_up, w_gate.T, w_up.T, 2)

        hidden, d_act_b = lax.optimization_barrier((hidden, d_act_b))
        out_part = jnp.dot(hidden, w_down, preferred_element_type=F32)
        out_mine = lax.psum_scatter(out_part, "tp", scatter_dimension=0, tiled=True)

        grad_down = jnp.einsum("tf,td->fd", hidden, dy, preferred_element_type=F32)
        grad_gate = jnp.einsum("tf,td->fd", d_gate, act_b, preferred_element_type=F32)
        grad_up = jnp.einsum("tf,td->fd", d_up, act_b, preferred_element_type=F32)
        d_act_b = d_act_b.astype(F32)
        grad_gain_b = jnp.sum(d_act_b * normed_b, axis=0)
        d_resid = dy.astype(F32) + rms_back(d_act_b * gain_b, normed_b, inv_b)
        d_resid_b = d_resid.astype(BF16)
        grad_out = jnp.einsum("tc,td->cd", attended, d_resid_b, preferred_element_type=F32)
        d_att = jnp.einsum("td,cd->tc", d_resid_b, w_o, preferred_element_type=F32).astype(BF16)
        d_q_pre, d_key_all, d_value_all = attention_back(query, key_all, value_all, d_att, lse, pos, cosine, sine)
        grad_q = jnp.einsum("td,tc->dc", act_a, d_q_pre, preferred_element_type=F32)
        early = (grad_gate, grad_up, grad_down, grad_q, grad_out)
        out_mine, d_q_pre, early, (ids, order, starts) = lax.optimization_barrier((out_mine, d_q_pre, early, (ids, order, starts)))
        early = lax.psum(early, "cp")
        d_embed, grad_gain_a, grad_gain_b, d_k_pre, d_v_pre = grad_a(
            d_q_pre, d_key_all, d_value_all, w_q, w_k, w_v, cosine, sine, embed_b, gain_a[None, :], grad_gain_b[None, :],
            d_resid, cp_count, 3)
        out_mine, d_embed, early = lax.optimization_barrier((out_mine, d_embed, early))
        res_mine = lax.dynamic_slice_in_dim(residual, tp_rank * (span // 4), span // 4, axis=0)
        layer_out = lax.all_gather((out_mine + res_mine).astype(BF16), "tp", axis=0, tiled=True)
        grad_k = jnp.einsum("td,tc->dc", act_all, d_k_pre, preferred_element_type=F32)
        grad_v = jnp.einsum("td,tc->dc", act_all, d_v_pre, preferred_element_type=F32)
        grad_table, grad_gate, grad_up, grad_down, grad_q, grad_out = table_grad(ids, order, starts, d_embed, rows, early)
        return (
            layer_out, grad_table, grad_q, grad_k, grad_v, grad_out, grad_gate.T, grad_up.T, grad_down, grad_gain_a[0], grad_gain_b[0])

    col_spec = P(None, "tp")
    row_spec = P("tp", None)
    tok_spec = P("cp")
    rep_spec = P(None)
    in_specs = (tok_spec, tok_spec, tok_spec, P("cp", None), row_spec, col_spec, col_spec, col_spec, row_spec, col_spec, col_spec, row_spec, rep_spec, rep_spec, rep_spec)
    out_specs = (P("cp", None), row_spec, col_spec, col_spec, col_spec, row_spec, col_spec, col_spec, row_spec, rep_spec, rep_spec)
    return jax.shard_map(device_step, mesh=mesh, in_specs=in_specs, out_specs=out_specs, check_vma=False)
```

```python
import functools

import jax
import jax.numpy as jnp
from jax import lax
from jax.experimental import pallas as pl
from jax.experimental.pallas import tpu as pltpu
from jax.sharding import PartitionSpec as P


NORM_EPS = 1e-5
NEG_BIG = -1e30
MESH = pl.DeviceIdType.MESH
NN = (((1,), (0,)), ((), ()))
NT = (((1,), (1,)), ((), ()))
VMEM_LIMIT = 60 * 1024 * 1024
F32 = jnp.float32
BF16 = jnp.bfloat16


def rms_stats(feats):
    inv_rms = lax.rsqrt(jnp.mean(feats * feats, axis=-1, keepdims=True) + NORM_EPS)
    return feats * inv_rms, inv_rms


def rms_back(d_normed, normed, inv_rms):
    return inv_rms * (d_normed - normed * jnp.mean(d_normed * normed, axis=-1, keepdims=True))


def to_bf16(feats):
    return feats.astype(BF16).astype(F32)


def neighbours():
    me = lax.axis_index("tp")
    return me, me + 1 - 2 * lax.rem(me, 2), lax.rem(me + 2, 4), 3 - me


def enter(peers):
    barrier = pltpu.get_barrier_semaphore()
    for peer in peers:
        pl.semaphore_signal(barrier, inc=1, device_id={"tp": peer}, device_id_type=MESH)
    pl.semaphore_wait(barrier, len(peers))


def remote(src, dst, sems, slot, peer):
    return pltpu.make_async_remote_copy(
        src_ref=src, dst_ref=dst, send_sem=sems.at[0, slot], recv_sem=sems.at[1, slot],
        device_id={"tp": peer}, device_id_type=MESH)


def tp_exchange(compute, done, out_ref, part, recv1, recv2, sems):
    wide = part.dtype
    block, half = part.shape[2], part.shape[3]
    piece = block // 2
    me, x_peer, y_peer, diag = neighbours()
    peers = (x_peer, y_peer)
    sides = [slice(side * half, (side + 1) * half) for side in range(2)]
    order = [(sub, side) for sub in range(2) for side in range(2)]

    def place(owner, sub):
        return pl.ds(pl.multiple_of(owner * block + sub * piece, piece), piece)

    first = []
    for k in range(2):
        for side in range(2):
            owner = diag if k == 0 else peers[side]
            compute(side, owner)
            copy = remote(part.at[side, owner], recv1.at[side, k], sems, side * 2 + k, peers[side])
            copy.start()
            first.append(copy)
    for side in range(2):
        compute(side, peers[1 - side])
    for side in range(2):
        compute(side, me)
    second = []
    for n, (sub, side) in enumerate(order):
        if sub == 0:
            first[side].wait_recv()
        owner = peers[1 - side]
        rows = pl.ds(sub * piece, piece)
        part[side, owner, rows] = (part[side, owner, rows].astype(F32) + recv1[side, 0, rows].astype(F32)).astype(wide)
        copy = remote(part.at[side, owner, rows], recv2.at[side, rows], sems, 4 + n, peers[1 - side])
        copy.start()
        second.append(copy)
    own = []
    for n, (sub, side) in enumerate(order):
        if sub == 0:
            first[2 + side].wait_recv()
        second[n].wait_recv()
        rows = pl.ds(sub * piece, piece)
        total = part[side, me, rows].astype(F32) + recv1[side, 1, rows].astype(F32) + recv2[side, rows].astype(F32)
        target = out_ref.at[place(me, sub), sides[side]]
        target[...] = total.astype(out_ref.dtype)
        copy = remote(target, target, sems, 8 + n, peers[1 - side])
        copy.start()
        own.append(copy)
    far = []
    for n, (sub, side) in enumerate(order):
        target = out_ref.at[place(me, sub), sides[side]]
        copy = remote(target, target, sems, 12 + n, peers[side])
        copy.start()
        far.append(copy)
    done(me)
    for n, (sub, side) in enumerate(order):
        own[n].wait_recv()
        target = out_ref.at[place(peers[1 - side], sub), sides[side]]
        copy = remote(target, target, sems, 16 + n, peers[side])
        copy.start()
        far.append(copy)
    for n in range(4):
        far[n].wait_recv()
    done(x_peer)
    done(y_peer)
    for n in range(4):
        far[4 + n].wait_recv()
    done(diag)
    for copy in first + second + own + far:
        copy.wait_send()


def exchange_scratch(span, width, wide):
    block, half = span // 4, width // 2
    return [
        pltpu.VMEM((2, 4, block, half), wide),
        pltpu.VMEM((2, 2, block, half), wide),
        pltpu.VMEM((2, block, half), wide),
        pltpu.SemaphoreType.DMA((2, 20)),
    ]


EXCHANGE_COST = pl.CostEstimate(flops=10**11, bytes_accessed=10**8, transcendentals=0)


def comm_params(collective_id, mib=60):
    return pltpu.CompilerParams(collective_id=collective_id, has_side_effects=True, vmem_limit_bytes=mib * 1024 * 1024)


VMEM_SPEC = pl.BlockSpec(memory_space=pltpu.VMEM)


def product_into(part, lhs, rhs, dims, bases):
    block, half = part.shape[2], part.shape[3]
    tile = 256

    def compute(side, owner):

        def step(j, carry):
            total = None
            for left, right, base in zip(lhs, rhs, bases):
                rows = pl.ds(pl.multiple_of(base + owner * block, block), block)
                start = pl.multiple_of(side * half + j * tile, tile)
                piece = right[pl.ds(start, tile), :] if dims == NT else right[:, pl.ds(start, tile)]
                term = lax.dot_general(left[rows, :], piece, dims, preferred_element_type=F32)
                total = term if total is None else total + term
            part[side, owner, :, pl.ds(pl.multiple_of(j * tile, tile), tile)] = total
            return carry

        lax.fori_loop(0, half // tile, step, 0)

    return compute


def inverse_root(value):
    guess = lax.rsqrt(value)
    return guess * (1.5 - 0.5 * value * guess * guess)


def turn(feats, cosine, sine):
    return feats * cosine + pltpu.roll(feats, feats.shape[-1] // 2, 1) * sine


def embed_kernel(picked, owned, gain, w_q_hbm, w_k_hbm, w_v_hbm, cosine, sine, embed, act, q_ref, k_ref, v_ref, part, recv1, recv2, sems, kv_sems, w_q, w_k, w_v, load_sems):
    block, half = part.shape[2], part.shape[3]
    span = picked.shape[0]
    head = cosine.shape[1]
    me, x_peer, y_peer, diag = neighbours()
    cp = lax.axis_index("cp")
    loads = [
        pltpu.make_async_copy(source, target, load_sems.at[which])
        for which, (source, target) in enumerate(((w_q_hbm, w_q), (w_k_hbm, w_k), (w_v_hbm, w_v)))]
    for copy in loads:
        copy.start()
    barrier = pltpu.get_barrier_semaphore()
    for peer in ({"tp": x_peer}, {"tp": y_peer}, {"cp": 1 - cp}):
        pl.semaphore_signal(barrier, inc=1, device_id=peer, device_id_type=MESH)
    pl.semaphore_wait(barrier, 3)
    sent = []

    def compute(side, owner):
        rows = pl.ds(pl.multiple_of(owner * block, block), block)
        part[side, owner] = (picked[rows, side * half:(side + 1) * half].astype(F32) * owned[rows, :]).astype(BF16)

    def done(owner):
        if not sent:
            for copy in loads:
                copy.wait()
        rows = pl.ds(pl.multiple_of(owner * block, block), block)
        slots = pl.ds(pl.multiple_of(cp * span + owner * block, block), block)
        feats = embed[rows, :].astype(F32)
        inv_rms = inverse_root(jnp.mean(feats * feats, axis=-1, keepdims=True) + NORM_EPS)
        act[rows, :] = (feats * inv_rms * gain[...]).astype(BF16)

        def step(j, carry):
            cols = pl.ds(pl.multiple_of(j * head, head), head)
            left = act[rows, :]
            query = jnp.dot(left, w_q[:, cols], preferred_element_type=F32)
            q_ref[rows, cols] = turn(query, cosine[rows, :], sine[rows, :]).astype(BF16)
            key = jnp.dot(left, w_k[:, cols], preferred_element_type=F32)
            k_ref[slots, cols] = turn(key, cosine[rows, :], sine[rows, :]).astype(BF16)
            v_ref[slots, cols] = jnp.dot(left, w_v[:, cols], preferred_element_type=F32).astype(BF16)
            return carry

        lax.fori_loop(0, w_q.shape[1] // head, step, 0)
        for ref in (k_ref, v_ref):
            slot = len(sent)
            copy = pltpu.make_async_remote_copy(
                src_ref=ref.at[slots], dst_ref=ref.at[slots], send_sem=kv_sems.at[0, slot], recv_sem=kv_sems.at[1, slot],
                device_id={"cp": 1 - cp}, device_id_type=MESH)
            copy.start()
            sent.append(copy)

    tp_exchange(compute, done, embed, part, recv1, recv2, sems)
    for copy in sent:
        copy.wait_recv()
    for copy in sent:
        copy.wait_send()


def embed_qkv(picked, owned, gain, w_q, w_k, w_v, cosine, sine, cp_count, collective_id):
    span, width = picked.shape
    cols = w_q.shape[1]
    return pl.pallas_call(
        embed_kernel,
        out_shape=[jax.ShapeDtypeStruct(shape, BF16) for shape in (
            (span, width), (span, width), (span, cols), (span * cp_count, cols), (span * cp_count, cols))],
        in_specs=[VMEM_SPEC] * 3 + [pl.BlockSpec(memory_space=pl.ANY)] * 3 + [VMEM_SPEC] * 2,
        out_specs=[VMEM_SPEC] * 5,
        scratch_shapes=exchange_scratch(span, width, BF16) + [pltpu.SemaphoreType.DMA((2, 8))]
        + [pltpu.VMEM(w_q.shape, BF16)] * 3 + [pltpu.SemaphoreType.DMA((3,))],
        compiler_params=comm_params(collective_id, 40),
        cost_estimate=EXCHANGE_COST,
        name="embed_qkv",
    )(picked, owned, gain, w_q, w_k, w_v, cosine, sine)


def grad_b_kernel(d_gate, d_up, w_gate, w_up, out, part, recv1, recv2, sems):
    enter(neighbours()[1:3])
    tp_exchange(product_into(part, (d_gate, d_up), (w_gate, w_up), NN, (0, 0)), lambda owner: None, out, part, recv1, recv2, sems)


def grad_b(d_gate, d_up, w_gate_t, w_up_t, collective_id):
    span, width = d_gate.shape[0], w_gate_t.shape[1]
    return pl.pallas_call(
        grad_b_kernel,
        out_shape=jax.ShapeDtypeStruct((span, width), BF16),
        in_specs=[VMEM_SPEC] * 4,
        out_specs=VMEM_SPEC,
        scratch_shapes=exchange_scratch(span, width, F32),
        compiler_params=comm_params(collective_id, 42),
        cost_estimate=EXCHANGE_COST,
        name="grad_b",
    )(d_gate, d_up, w_gate_t, w_up_t)


def grad_a_kernel(
    d_q, d_k_all, d_v_all, w_q, w_k, w_v, cosine, sine, embed_hbm, gain, gain_b_part, d_resid,
    d_embed, grad_gain, grad_gain_b, d_k, d_v, out, resid, recv_k, recv_v, part, recv1, recv2, sems, kv_sems, row_sems, gain_part, gain_other, own_k, own_v, embed):
    span = d_q.shape[0]
    block = part.shape[2]
    head = cosine.shape[1]
    me, x_peer, y_peer, diag = neighbours()
    cp = lax.axis_index("cp")
    barrier = pltpu.get_barrier_semaphore()
    for peer in ({"tp": x_peer}, {"tp": y_peer}, {"cp": 1 - cp}):
        pl.semaphore_signal(barrier, inc=1, device_id=peer, device_id_type=MESH)
    pl.semaphore_wait(barrier, 3)
    late_loads = [
        pltpu.make_async_copy(d_resid, resid, row_sems.at[0, 0]), pltpu.make_async_copy(embed_hbm, embed, row_sems.at[1, 0])]
    held = pl.ds(pl.multiple_of(cp * span, span), span)
    loads = [
        pltpu.make_async_copy(source.at[held], target, row_sems.at[3, 2 + which])
        for which, (source, target) in enumerate(((d_k_all, own_k), (d_v_all, own_v)))]
    for copy in loads + late_loads:
        copy.start()
    trades = []
    for which, source in enumerate((gain_b_part, gain_part)):
        trades.append(pltpu.make_async_remote_copy(
            src_ref=source, dst_ref=gain_other.at[which], send_sem=row_sems.at[3, which], recv_sem=row_sems.at[4, which],
            device_id={"cp": 1 - cp}, device_id_type=MESH))
    trades[0].start()
    order = (diag, x_peer, y_peer, me)
    copies = []
    for place, owner in enumerate(order):
        rows = pl.ds(pl.multiple_of(owner * block, block), block)
        theirs = pl.ds(pl.multiple_of((1 - cp) * span + owner * block, block), block)
        for which, (source, target) in enumerate(((d_k_all, recv_k), (d_v_all, recv_v))):
            slot = 2 * place + which
            copy = pltpu.make_async_remote_copy(
                src_ref=source.at[theirs], dst_ref=target.at[rows], send_sem=kv_sems.at[0, slot], recv_sem=kv_sems.at[1, slot],
                device_id={"cp": 1 - cp}, device_id_type=MESH)
            copy.start()
            copies.append(copy)
    product = product_into(part, (d_q, d_k, d_v), (w_q, w_k, w_v), NT, (0, cp * span, cp * span))
    ready = []

    def prepare(place):
        owner = order[place]
        if place == 0:
            for copy in loads:
                copy.wait()
        copies[2 * place].wait_recv()
        copies[2 * place + 1].wait_recv()
        rows = pl.ds(pl.multiple_of(owner * block, block), block)
        ours = pl.ds(pl.multiple_of(cp * span + owner * block, block), block)

        def step(j, carry):
            cols = pl.ds(pl.multiple_of(j * head, head), head)
            total = (own_k[rows, cols] + recv_k[rows, cols]).astype(BF16).astype(F32)
            d_k[ours, cols] = turn(total, cosine[rows, :], -sine[rows, :]).astype(BF16)
            d_v[ours, cols] = (own_v[rows, cols] + recv_v[rows, cols]).astype(BF16)
            return carry

        lax.fori_loop(0, d_q.shape[1] // head, step, 0)
        for which, ref in enumerate((d_k, d_v)):
            slot = 8 + 2 * place + which
            copy = pltpu.make_async_remote_copy(
                src_ref=ref.at[ours], dst_ref=ref.at[ours], send_sem=kv_sems.at[0, slot], recv_sem=kv_sems.at[1, slot],
                device_id={"cp": 1 - cp}, device_id_type=MESH)
            copy.start()
            ready.append(copy)

    calls = []

    def compute(side, owner):
        turn_no = len(calls)
        calls.append(side)
        if turn_no == 0:
            prepare(0)
        elif turn_no == 2:
            prepare(1)
        elif turn_no == 3:
            prepare(2)
        elif turn_no == 6:
            prepare(3)
        product(side, owner)

    gain_part[...] = jnp.zeros_like(gain_part)
    local, shared = [], []

    def done(owner):
        if not local:
            for copy in late_loads:
                copy.wait()
        rows = pl.ds(pl.multiple_of(owner * block, block), block)
        slots = pl.ds(pl.multiple_of(cp * span + owner * block, block), block)
        feats = embed[rows, :].astype(F32)
        inv_rms = inverse_root(jnp.mean(feats * feats, axis=-1, keepdims=True) + NORM_EPS)
        normed = feats * inv_rms
        d_act = out[rows, :].astype(F32)
        gain_part[...] = gain_part[...] + jnp.sum(d_act * normed, axis=0, keepdims=True)
        resid[rows, :] = resid[rows, :] + rms_back(d_act * gain[...], normed, inv_rms)
        slot = 1 + len(local)
        copy = pltpu.make_async_copy(resid.at[rows], d_embed.at[slots], row_sems.at[0, slot])
        copy.start()
        local.append(copy)
        copy = pltpu.make_async_remote_copy(
            src_ref=resid.at[rows], dst_ref=d_embed.at[slots], send_sem=row_sems.at[1, slot], recv_sem=row_sems.at[2, slot],
            device_id={"cp": 1 - cp}, device_id_type=MESH)
        copy.start()
        shared.append(copy)

    tp_exchange(compute, done, out, part, recv1, recv2, sems)
    trades[1].start()
    for copy in local:
        copy.wait()
    for copy in trades:
        copy.wait_recv()
    grad_gain[...] = gain_part[...] + gain_other[1]
    grad_gain_b[...] = gain_b_part[...] + gain_other[0]
    for copy in shared + ready:
        copy.wait_recv()
    for copy in copies + shared + ready + trades:
        copy.wait_send()


def grad_a(d_q, d_k_all, d_v_all, w_q, w_k, w_v, cosine, sine, embed, gain, gain_b_part, d_resid, cp_count, collective_id):
    span, width = d_q.shape[0], w_q.shape[0]
    cols = d_q.shape[1]
    hbm = pl.BlockSpec(memory_space=pl.ANY)
    return pl.pallas_call(
        grad_a_kernel,
        out_shape=[
            jax.ShapeDtypeStruct((span * cp_count, width), F32), jax.ShapeDtypeStruct((1, width), F32),
            jax.ShapeDtypeStruct((1, width), F32)] + [jax.ShapeDtypeStruct((span * cp_count, cols), BF16)] * 2,
        in_specs=[VMEM_SPEC] + [hbm] * 2 + [VMEM_SPEC] * 5 + [hbm] + [VMEM_SPEC] * 2 + [hbm],
        out_specs=[hbm] + [VMEM_SPEC] * 4,
        scratch_shapes=[pltpu.VMEM((span, width), BF16), pltpu.VMEM((span, width), F32)] + [pltpu.VMEM((span, cols), F32)] * 2
        + exchange_scratch(span, width, F32) + [pltpu.SemaphoreType.DMA((2, 16)), pltpu.SemaphoreType.DMA((5, 5))]
        + [pltpu.VMEM((1, width), F32), pltpu.VMEM((2, 1, width), F32)]
        + [pltpu.VMEM((span, cols), F32)] * 2 + [pltpu.VMEM((span, width), BF16)],
        compiler_params=comm_params(collective_id),
        cost_estimate=EXCHANGE_COST,
        name="grad_a",
    )(d_q, d_k_all, d_v_all, w_q, w_k, w_v, cosine, sine, embed, gain, gain_b_part, d_resid)


Q_TILE = 256


def key_row(chunk, size):
    return pl.multiple_of(jnp.where(chunk < 2, 2 * chunk, 7 - 2 * chunk) * size, size)


def query_plan(i, size, pos_smem):
    cp = lax.axis_index("cp")
    per_block = size // Q_TILE
    seq_block = jnp.where(i < per_block, cp, 3 - cp)
    start = seq_block * size + lax.rem(i, per_block) * Q_TILE
    low = jnp.maximum(start - pos_smem[i * Q_TILE], 0) // size
    return start, low, seq_block + 1


def distance(size):
    return lax.broadcasted_iota(jnp.int32, (Q_TILE, size), 0) - lax.broadcasted_iota(jnp.int32, (Q_TILE, size), 1)


def attend_kernel(pos_smem, q_ref, k_ref, v_ref, pos_ref, o_ref, lse_ref, held, tops):
    size = held.shape[2]
    head = q_ref.shape[1]
    scale = head ** -0.5

    def block(i, carry):
        start, low, high = query_plan(i, size, pos_smem)
        rows = pl.ds(pl.multiple_of(i * Q_TILE, Q_TILE), Q_TILE)
        query = q_ref[rows, :]
        back = pos_ref[rows, :]

        def score(c, carry):
            top, total = carry
            keys = k_ref[pl.ds(key_row(c, size), size), :]
            scores = lax.dot_general(query, keys, NT, preferred_element_type=F32) * scale
            gap = distance(size) + (start - c * size)
            scores = jnp.where((gap >= 0) & (gap <= back), scores, NEG_BIG)
            risen = jnp.maximum(top, jnp.max(scores, axis=1, keepdims=True))
            prob = jnp.exp(scores - risen)
            held[c] = prob
            tops[c] = risen
            return risen, total * jnp.exp(top - risen) + jnp.sum(prob, axis=1, keepdims=True)

        top, total = lax.fori_loop(
            low, high, score, (jnp.full((Q_TILE, 1), NEG_BIG, F32), jnp.zeros((Q_TILE, 1), F32)))
        share = 1.0 / total

        def gather(c, acc):
            prob = (held[c] * (jnp.exp(tops[c] - top) * share)).astype(BF16)
            values = v_ref[pl.ds(key_row(c, size), size), :]
            return acc + jnp.dot(prob, values, preferred_element_type=F32)

        acc = lax.fori_loop(low, high, gather, jnp.zeros((Q_TILE, head), F32))
        o_ref[rows, :] = acc.astype(BF16)
        lse_ref[rows, :] = jnp.broadcast_to(top + jnp.log(total), (Q_TILE, head))
        return carry

    lax.fori_loop(0, q_ref.shape[0] // Q_TILE, block, 0)


def attend_back_kernel(pos_smem, q_ref, k_ref, v_ref, do_ref, lse_ref, pos_ref, cosine, sine, dq_ref, dk_ref, dv_ref, held_p, held_d):
    size = held_p.shape[2]
    head = q_ref.shape[1]
    scale = head ** -0.5
    dk_ref[...] = jnp.zeros_like(dk_ref)
    dv_ref[...] = jnp.zeros_like(dv_ref)
    over_rows = (((0,), (0,)), ((), ()))

    def block(i, carry):
        start, low, high = query_plan(i, size, pos_smem)
        rows = pl.ds(pl.multiple_of(i * Q_TILE, Q_TILE), Q_TILE)
        query = q_ref[rows, :]
        d_out = do_ref[rows, :]
        lse = lse_ref[rows, :][:, :1]
        back = pos_ref[rows, :]

        def probs(c, total):
            place = pl.ds(key_row(c, size), size)
            scores = lax.dot_general(query, k_ref[place, :], NT, preferred_element_type=F32) * scale
            gap = distance(size) + (start - c * size)
            prob = jnp.where((gap >= 0) & (gap <= back), jnp.exp(scores - lse), 0.0)
            d_prob = to_bf16(lax.dot_general(d_out, v_ref[place, :], NT, preferred_element_type=F32))
            held_p[c] = prob
            held_d[c] = d_prob
            return total + jnp.sum(prob * d_prob, axis=1, keepdims=True)

        mean = lax.fori_loop(low, high, probs, jnp.zeros((Q_TILE, 1), F32))

        def grads(c, acc):
            place = pl.ds(key_row(c, size), size)
            prob = held_p[c]
            d_score = (prob * (held_d[c] - mean) * scale).astype(BF16)
            dk_ref[place, :] = dk_ref[place, :] + lax.dot_general(d_score, query, over_rows, preferred_element_type=F32)
            dv_ref[place, :] = dv_ref[place, :] + lax.dot_general(prob.astype(BF16), d_out, over_rows, preferred_element_type=F32)
            return acc + jnp.dot(d_score, k_ref[place, :], preferred_element_type=F32)

        d_query = lax.fori_loop(low, high, grads, jnp.zeros((Q_TILE, head), F32))
        dq_ref[rows, :] = turn(to_bf16(d_query), cosine[rows, :], -sine[rows, :]).astype(BF16)
        return carry

    lax.fori_loop(0, q_ref.shape[0] // Q_TILE, block, 0)


def attention(query, key_all, value_all, pos, head):
    span, cols = query.shape
    total = key_all.shape[0]
    size = total // 4
    own = pl.BlockSpec((span, head), lambda h, *_: (0, h))
    full = pl.BlockSpec((total, head), lambda h, *_: (0, h))
    pos_spec = pl.BlockSpec((span, 1), lambda h, *_: (0, 0))
    flops = 4 * span * total * cols
    return pl.pallas_call(
        attend_kernel,
        grid_spec=pltpu.PrefetchScalarGridSpec(
            num_scalar_prefetch=1, grid=(cols // head,), in_specs=[own, full, full, pos_spec], out_specs=[own, own],
            scratch_shapes=[pltpu.VMEM((4, Q_TILE, size), F32), pltpu.VMEM((4, Q_TILE, 1), F32)]),
        out_shape=[jax.ShapeDtypeStruct((span, cols), BF16), jax.ShapeDtypeStruct((span, cols), F32)],
        cost_estimate=pl.CostEstimate(flops=flops, bytes_accessed=8 * total * cols, transcendentals=0),
        compiler_params=pltpu.CompilerParams(vmem_limit_bytes=VMEM_LIMIT // 2),
        name="attention",
    )(pos, query, key_all, value_all, pos[:, None])


def attention_back(query, key_all, value_all, d_att, lse, pos, cosine, sine):
    span, cols = query.shape
    head = cosine.shape[1]
    total = key_all.shape[0]
    size = total // 4
    own = pl.BlockSpec((span, head), lambda h, *_: (0, h))
    full = pl.BlockSpec((total, head), lambda h, *_: (0, h))
    same = pl.BlockSpec((span, head), lambda h, *_: (0, 0))
    pos_spec = pl.BlockSpec((span, 1), lambda h, *_: (0, 0))
    flops = 10 * span * total * cols
    return pl.pallas_call(
        attend_back_kernel,
        grid_spec=pltpu.PrefetchScalarGridSpec(
            num_scalar_prefetch=1, grid=(cols // head,),
            in_specs=[own, full, full, own, own, pos_spec, same, same], out_specs=[own, full, full],
            scratch_shapes=[pltpu.VMEM((4, Q_TILE, size), F32)] * 2),
        out_shape=[jax.ShapeDtypeStruct((span, cols), BF16)] + [jax.ShapeDtypeStruct((total, cols), F32)] * 2,
        cost_estimate=pl.CostEstimate(flops=flops, bytes_accessed=16 * total * cols, transcendentals=0),
        compiler_params=pltpu.CompilerParams(vmem_limit_bytes=VMEM_LIMIT // 2),
        name="attention_back",
    )(pos, query, key_all, value_all, d_att, lse, pos[:, None], cosine, sine)


ROW_TILE = 200


PASS_TILES = 16


def table_kernel(count, start, order, ids, source, *refs):
    passed, out_ref, written, grads, sem = refs[:count], refs[count], refs[count + 1:2 * count + 1], refs[-2], refs[-1]
    step = pl.program_id(0)

    @pl.when(step == 0)
    def _():
        copy = pltpu.make_async_copy(source, grads, sem)
        copy.start()
        copy.wait()

    @pl.when(step < PASS_TILES)
    def _():
        for left, right in zip(passed, written):
            right[...] = left[...]

    out_ref[...] = jnp.zeros_like(out_ref)
    base = step * out_ref.shape[0]

    def add(i, carry):
        row = pl.ds(ids[i] - base, 1)
        out_ref[row, :] = out_ref[row, :] + grads[pl.ds(order[i], 1), :]
        return carry

    lax.fori_loop(start[step], start[step + 1], add, 0)


def table_grad(ids, order, start, source, rows, passed):
    total, width = source.shape
    tiles = rows // ROW_TILE
    specs = []
    for array in passed:
        if array.shape[1] == width:
            specs.append(pl.BlockSpec((array.shape[0], width // PASS_TILES), lambda i, *_: (0, jnp.minimum(i, PASS_TILES - 1))))
        else:
            specs.append(pl.BlockSpec((array.shape[0] // PASS_TILES, array.shape[1]), lambda i, *_: (jnp.minimum(i, PASS_TILES - 1), 0)))
    return pl.pallas_call(
        functools.partial(table_kernel, len(passed)),
        grid_spec=pltpu.PrefetchScalarGridSpec(
            num_scalar_prefetch=3, grid=(tiles,), in_specs=[pl.BlockSpec(memory_space=pl.ANY)] + specs,
            out_specs=[pl.BlockSpec((ROW_TILE, width), lambda i, *_: (i, 0))] + specs,
            scratch_shapes=[pltpu.VMEM((total, width), F32), pltpu.SemaphoreType.DMA]),
        out_shape=[jax.ShapeDtypeStruct((rows, width), F32)] + [jax.ShapeDtypeStruct(array.shape, F32) for array in passed],
        cost_estimate=pl.CostEstimate(flops=4 * 10**10, bytes_accessed=4 * rows * width, transcendentals=0),
        compiler_params=pltpu.CompilerParams(vmem_limit_bytes=VMEM_LIMIT * 3 // 4),
        name="table_grad",
    )(start, order, ids, source, *passed)


def out_proj_kernel(att_ref, w_mine, w_other, embed_ref, dy_hbm, w_down_hbm, res_ref, d_hidden, slots, sems, dy_ref, w_down, load_sems):
    me, x_peer, y_peer, diag = neighbours()
    peers = (x_peer, y_peer)
    loads = [
        pltpu.make_async_copy(source, target, load_sems.at[which])
        for which, (source, target) in enumerate(((dy_hbm, dy_ref), (w_down_hbm, w_down)))]
    for copy in loads:
        copy.start()
    enter(peers)
    width = att_ref.shape[1]
    half = att_ref.shape[0] // 2
    sides = [pl.ds(0, half), pl.ds(half, half)]

    cp = lax.axis_index("cp")
    part = w_mine.shape[1]
    tile = 256

    def multiply(block, owner, initial):
        rows = pl.ds(pl.multiple_of(owner * width, width), width)
        for w_ref, base in ((w_mine, cp), (w_other, 1 - cp)):

            def step(j, carry):
                cols = pl.ds(pl.multiple_of(base * part + j * tile, tile), tile)
                term = jnp.dot(block[...], w_ref[rows, pl.ds(pl.multiple_of(j * tile, tile), tile)], preferred_element_type=F32)
                before = embed_ref[:, cols].astype(F32) if initial else res_ref[:, cols]
                res_ref[:, cols] = before + term
                return carry

            lax.fori_loop(0, part // tile, step, 0)

    near = []
    for side in range(2):
        copy = remote(att_ref.at[sides[side]], slots.at[me, sides[side]], sems, side, peers[side])
        copy.start()
        near.append(copy)
    far = []
    for side in range(2):
        copy = remote(att_ref.at[sides[side]], slots.at[me, sides[side]], sems, 2 + side, peers[1 - side])
        copy.start()
        far.append(copy)
    multiply(att_ref, me, True)
    last = []
    for side in range(2):
        near[side].wait_recv()
        owner = peers[side]
        copy = remote(slots.at[owner, sides[side]], slots.at[owner, sides[side]], sems, 4 + side, peers[1 - side])
        copy.start()
        last.append(copy)

    def back(i, carry):
        rows = pl.ds(pl.multiple_of(i * 128, 128), 128)
        d_hidden[rows, :] = lax.dot_general(dy_ref[rows, :], w_down[...], NT, preferred_element_type=F32).astype(BF16)
        return carry

    for copy in loads:
        copy.wait()
    lax.fori_loop(0, dy_ref.shape[0] // 128, back, 0)
    for side in range(2):
        far[side].wait_recv()
    for side in range(2):
        multiply(slots.at[peers[side]], peers[side], False)
    for side in range(2):
        last[side].wait_recv()
    multiply(slots.at[diag], diag, False)
    for copy in near + far + last:
        copy.wait_send()


def out_proj(attended, w_mine, w_other, embed, dy, w_down, collective_id):
    span, width = attended.shape
    return pl.pallas_call(
        out_proj_kernel,
        out_shape=[jax.ShapeDtypeStruct(embed.shape, F32), jax.ShapeDtypeStruct((span, w_down.shape[0]), BF16)],
        in_specs=[VMEM_SPEC] * 4 + [pl.BlockSpec(memory_space=pl.ANY)] * 2,
        out_specs=[VMEM_SPEC] * 2,
        scratch_shapes=[
            pltpu.VMEM((4, span, width), BF16), pltpu.SemaphoreType.DMA((2, 6)), pltpu.VMEM(dy.shape, BF16),
            pltpu.VMEM(w_down.shape, BF16), pltpu.SemaphoreType.DMA((2,))],
        compiler_params=comm_params(collective_id, 46),
        cost_estimate=EXCHANGE_COST,
        name="out_proj",
    )(attended, w_mine, w_other, embed, dy, w_down)


def solution(mesh):
    cp_count = mesh.shape["cp"]

    def device_step(tokens, pos, doc_id, dy, table, w_q, w_k, w_v, w_o, w_gate, w_up, w_down, gain_one, gain_two, inv_freq):
        span = tokens.shape[0]
        rows = table.shape[0]
        head_dim = 2 * inv_freq.shape[0]
        tp_rank = lax.axis_index("tp")
        gain_a = gain_one.astype(F32)
        gain_b = gain_two.astype(F32)
        swap = [(0, 1), (1, 0)]

        local_ids = tokens - tp_rank * rows
        owned = (local_ids >= 0) & (local_ids < rows)
        safe_ids = jnp.where(owned, local_ids, jnp.arange(span, dtype=jnp.int32) % rows)
        picked = jnp.take(table, safe_ids, axis=0, mode="clip")
        half_width = w_o.shape[1] // cp_count
        w_o_half = lax.dynamic_slice_in_dim(w_o, lax.axis_index("cp") * half_width, half_width, axis=1)
        w_o_mine = lax.all_gather(w_o_half, "tp", axis=0, tiled=True)
        all_ids = lax.all_gather(tokens, "cp", axis=0, tiled=True) - tp_rank * rows
        all_ids = jnp.where((all_ids >= 0) & (all_ids < rows), all_ids, rows)
        ids, order = lax.sort((all_ids, jnp.arange(all_ids.shape[0], dtype=jnp.int32)), num_keys=1, is_stable=True)
        edges = jnp.arange(rows // ROW_TILE + 1, dtype=jnp.int32) * ROW_TILE
        starts = jnp.sum((all_ids[None, :] < edges[:, None]).astype(jnp.int32), axis=1)
        angle = pos.astype(F32)[:, None] * inv_freq
        cosine, sine = jnp.cos(angle), jnp.sin(angle)
        cosine = jnp.concatenate([cosine, cosine], axis=1)
        sine = jnp.concatenate([-sine, sine], axis=1)
        embed_b, act_a, query, key_all, value_all = embed_qkv(
            picked, owned.astype(F32)[:, None], gain_a[None, :], w_q, w_k, w_v, cosine, sine, cp_count, 0)
        w_o_mine, query, act_a = lax.optimization_barrier((w_o_mine, query, act_a))
        act_all = lax.all_gather(act_a, "cp", axis=0, tiled=True)
        w_o_other = lax.ppermute(w_o_mine, "cp", swap)
        attended, lse = attention(query, key_all, value_all, pos, head_dim)
        residual, d_hidden = out_proj(attended, w_o_mine, w_o_other, embed_b, dy, w_down, 1)
        normed_b, inv_b = rms_stats(residual)
        act_b = (normed_b * gain_b).astype(BF16)
        gate = jnp.dot(act_b, w_gate, preferred_element_type=F32)
        up_val = jnp.dot(act_b, w_up, preferred_element_type=F32)
        gate_sig = jax.nn.sigmoid(gate)
        hidden = (gate * gate_sig * up_val).astype(BF16)
        d_hidden = d_hidden.astype(F32)
        d_gate = (d_hidden * up_val * gate_sig * (1.0 + gate * (1.0 - gate_sig))).astype(BF16)
        d_up = (d_hidden * gate * gate_sig).astype(BF16)
        d_act_b = grad_b(d_gate, d_up, w_gate.T, w_up.T, 2)

        hidden, d_act_b = lax.optimization_barrier((hidden, d_act_b))
        out_part = jnp.dot(hidden, w_down, preferred_element_type=F32)
        out_mine = lax.psum_scatter(out_part, "tp", scatter_dimension=0, tiled=True)

        grad_down = jnp.einsum("tf,td->fd", hidden, dy, preferred_element_type=F32)
        grad_gate = jnp.einsum("tf,td->fd", d_gate, act_b, preferred_element_type=F32)
        grad_up = jnp.einsum("tf,td->fd", d_up, act_b, preferred_element_type=F32)
        d_act_b = d_act_b.astype(F32)
        grad_gain_b = jnp.sum(d_act_b * normed_b, axis=0)
        d_resid = dy.astype(F32) + rms_back(d_act_b * gain_b, normed_b, inv_b)
        d_resid_b = d_resid.astype(BF16)
        grad_out = jnp.einsum("tc,td->cd", attended, d_resid_b, preferred_element_type=F32)
        d_att = jnp.einsum("td,cd->tc", d_resid_b, w_o, preferred_element_type=F32).astype(BF16)
        d_q_pre, d_key_all, d_value_all = attention_back(query, key_all, value_all, d_att, lse, pos, cosine, sine)
        grad_q = jnp.einsum("td,tc->dc", act_a, d_q_pre, preferred_element_type=F32)
        early = (grad_gate, grad_up, grad_down, grad_q, grad_out)
        out_mine, d_q_pre, early, (ids, order, starts) = lax.optimization_barrier((out_mine, d_q_pre, early, (ids, order, starts)))
        early = lax.psum(early, "cp")
        d_embed, grad_gain_a, grad_gain_b, d_k_pre, d_v_pre = grad_a(
            d_q_pre, d_key_all, d_value_all, w_q, w_k, w_v, cosine, sine, embed_b, gain_a[None, :], grad_gain_b[None, :],
            d_resid, cp_count, 3)
        out_mine, d_embed, early = lax.optimization_barrier((out_mine, d_embed, early))
        res_mine = lax.dynamic_slice_in_dim(residual, tp_rank * (span // 4), span // 4, axis=0)
        layer_out = lax.all_gather((out_mine + res_mine).astype(BF16), "tp", axis=0, tiled=True)
        grad_k = jnp.einsum("td,tc->dc", act_all, d_k_pre, preferred_element_type=F32)
        grad_v = jnp.einsum("td,tc->dc", act_all, d_v_pre, preferred_element_type=F32)
        grad_table, grad_gate, grad_up, grad_down, grad_q, grad_out = table_grad(ids, order, starts, d_embed, rows, early)
        return (
            layer_out, grad_table, grad_q, grad_k, grad_v, grad_out, grad_gate.T, grad_up.T, grad_down, grad_gain_a[0], grad_gain_b[0])

    col_spec = P(None, "tp")
    row_spec = P("tp", None)
    tok_spec = P("cp")
    rep_spec = P(None)
    in_specs = (tok_spec, tok_spec, tok_spec, P("cp", None), row_spec, col_spec, col_spec, col_spec, row_spec, col_spec, col_spec, row_spec, rep_spec, rep_spec, rep_spec)
    out_specs = (P("cp", None), row_spec, col_spec, col_spec, col_spec, row_spec, col_spec, col_spec, row_spec, rep_spec, rep_spec)
    return jax.shard_map(device_step, mesh=mesh, in_specs=in_specs, out_specs=out_specs, check_vma=False)
```
